128 devices in a mesh: seg: 32 (over y, z, core), grp: 4 (over x).
Axes of the slice: x: 4, y: 4, z: 4, core: 2. Of those that a mesh axis runs over, the one named last changes fastest.
Arguments:
- basis: float32 [8, 3072, 128], P(None, ('seg', 'grp')), may hold values from -6 to 6
- coords: float32 [3072, 3, 128], P(('seg', 'grp')), may hold values from 0 to 4
- areas: float32 [3072, 128], P(('seg', 'grp')), may hold values from 0.5 to 2
- p2m: bfloat16 [3072, 121, 128], P(('seg', 'grp')), may hold values from -0.5 to 0.5
- l2p: bfloat16 [3072, 128, 121], P(('seg', 'grp')), may hold values from -0.5 to 0.5
- m2l: bfloat16 [316, 121, 121], replicated, may hold values from -0.0390625 to 0.0390625
- counts: int32 [128], P(('seg', 'grp')), may hold values from 8 to 24
- near_list: int32 [3072, 27], P(('seg', 'grp')), may hold values from 0 to 287
- far_list: int32 [3072, 189], P(('seg', 'grp')), may hold values from 0 to 287
- far_offset: int32 [3072, 189], P(('seg', 'grp')), may hold values from 0 to 315
Outputs:
- new_vector: float32 [3072, 128], P(('seg', 'grp'))
- hessenberg: float32 [9], replicated
The draws below stay inside these ranges and needn't reach their ends.
Inputs may be any that keep to these rules, and one draw needn't show every extreme that they name: `near_list`: window indices follow the rule of the steps; entries may name empty slots or leaves beyond the ends of the curve, which contribute nothing. A device's live leaves are its first counts slots.
All inputs are finite; a program needn't handle non-finite values.
Results may differ from the reference program's by a relative error of at most 0.0012.
Values sent between devices are 32-bit elements; how exact they have to be, the bound alone decides.
A program may use at most 64 MiB of HBM per device.

```python
import math
import jax
import jax.numpy as jnp
from jax import lax

PAN = 128
TERMS = 121
OFFSETS = 316
FAR = 189
NEAR = 27
KRYLOV = 8
LEAF_DEV = 24
LEAVES = 3072
N_SEG = 32
N_GRP = 4


def draw_basis(key, part):
    first, second = jax.random.split(jax.random.fold_in(key, 17))
    separate = jnp.clip(jax.random.normal(first, (KRYLOV, LEAVES, PAN), jnp.float32), -4.0, 4.0)
    shared = jnp.clip(jax.random.normal(second, (1, LEAVES, PAN), jnp.float32), -4.0, 4.0)
    return 0.6 * separate + 0.8 * shared


def place_ends(entries, own_key, least, high):
    dims = entries.shape
    spot = [jax.random.randint(jax.random.fold_in(own_key, axis), (), 0, dims[axis]) for axis in range(len(dims))]
    entries = entries.at[tuple(spot)].set(least)
    longest = dims.index(max(dims))
    spot[longest] = (spot[longest] + 1) % dims[longest]
    return entries.at[tuple(spot)].set(high)


def steps_of(own_key, shape, cuts, smallest, top_value):
    def one(axis_at, parts):
        draws = jax.random.uniform(jax.random.fold_in(jax.random.fold_in(own_key, 6), axis_at), (parts,), jnp.float32, smallest / len(cuts), top_value / len(cuts))
        return jnp.repeat(jnp.exp(draws), shape[axis_at] // parts).reshape((-1,) + (1,) * (len(shape) - axis_at - 1))

    factor_of = one(*cuts[0])
    for cut in cuts[1:]:
        factor_of = factor_of * one(*cut)
    return factor_of


def bell_draw(rng, shape, scale, reach, shards=(), kind=jnp.bfloat16):
    result = scale * jax.random.normal(rng, shape, jnp.float32)
    if shards:
        result = result * steps_of(rng, shape, shards, -0.22, 0.18)
    return jnp.clip(result, -reach, reach).astype(kind)


def setup_inputs(seed: int = 0) -> dict:
    splits = jax.random.split(jax.random.key(seed), 11)
    basis = draw_basis(jax.random.fold_in(splits[10], 71), 0)
    coords = jnp.clip(4.0 * jax.random.uniform(splits[1], (LEAVES, 3, PAN), jnp.float32) ** steps_of(splits[1], (LEAVES, 3, PAN), ((0, 128),), -0.2, 0.2), 0.0, 4.0)
    areas = jnp.clip(jnp.exp(math.log(2.0) - 1.3862944 * jax.random.uniform(splits[2], (LEAVES, PAN), jnp.float32) ** steps_of(splits[2], (LEAVES, PAN), ((0, 128),), -0.2, 0.2)), 0.5, 2.0)
    p2m = bell_draw(splits[3], (LEAVES, TERMS, PAN), PAN ** -0.5, 0.5, ((0, 128),))
    l2p = bell_draw(splits[4], (LEAVES, PAN, TERMS), TERMS ** -0.5, 0.5, ((0, 128),))
    m2l = bell_draw(splits[5], (OFFSETS, TERMS, TERMS), (TERMS * FAR) ** -0.5, 0.0390625)
    counts = place_ends(jax.random.randint(splits[6], (N_SEG * N_GRP,), LEAF_DEV // 3, LEAF_DEV + 1), jax.random.fold_in(splits[6], 1), LEAF_DEV // 3, LEAF_DEV).astype(jnp.int32)
    near_list = place_ends(jax.random.randint(splits[7], (LEAVES, NEAR), 0, 3 * N_GRP * LEAF_DEV), jax.random.fold_in(splits[7], 1), 0, (3 * N_GRP * LEAF_DEV) - 1).astype(jnp.int32)
    far_list = place_ends(jax.random.randint(splits[8], (LEAVES, FAR), 0, 3 * N_GRP * LEAF_DEV), jax.random.fold_in(splits[8], 1), 0, (3 * N_GRP * LEAF_DEV) - 1).astype(jnp.int32)
    far_offset = place_ends(jax.random.randint(splits[9], (LEAVES, FAR), 0, OFFSETS), jax.random.fold_in(splits[9], 1), 0, OFFSETS - 1).astype(jnp.int32)
    return {"basis": basis, "coords": coords, "areas": areas, "p2m": p2m, "l2p": l2p, "m2l": m2l, "counts": counts, "near_list": near_list, "far_list": far_list, "far_offset": far_offset}


four_pi = 12.566370614359172
epsilon = 1e-06
highest = lax.Precision.HIGHEST

def live_slots(counts, leaves):
    leaf_dev = leaves // counts.shape[0]
    position = jnp.arange(leaves, dtype=jnp.int32)
    owner = position // leaf_dev
    return (position % leaf_dev < counts[owner]).astype(jnp.float32)[:, None]

def reference(basis, coords, areas, p2m, l2p, m2l, counts, near_list, far_list, far_offset):
    leaves, panels = areas.shape
    krylov = basis.shape[0]
    terms = m2l.shape[1]
    offsets = m2l.shape[0]
    far_count = far_list.shape[1]
    group = N_GRP * (leaves // counts.shape[0])
    live_mask = live_slots(counts, leaves)
    current = basis[krylov - 1] * live_mask
    rounded = current.astype(jnp.bfloat16)
    rounded = lax.optimization_barrier(rounded)
    multipoles = jnp.einsum('lkp,lp->lk', p2m.astype(jnp.float32), rounded.astype(jnp.float32), precision=highest)
    packed = jnp.concatenate([coords, areas[:, None, :], current[:, None, :]], axis=1)
    padded = jnp.pad(packed, ((group, group), (0, 0), (0, 0)))
    poles = jnp.pad(multipoles, ((group, group), (0, 0)))
    base_index = (jnp.arange(leaves, dtype=jnp.int32) // group * group)[:, None]
    near_rows = (base_index + near_list).astype(jnp.int32)
    far_rows = (base_index + far_list).astype(jnp.int32)
    table = m2l.astype(jnp.float32)

    def segment_work(leaf_block):
        target, near_block, far_block, offset_block = leaf_block

        def near_step(running, column):
            source = padded[column]
            square = jnp.zeros((group, panels, panels), jnp.float32)
            for component in range(3):
                spread = target[:, component, :, None] - source[:, component, None, :]
                square = square + spread * spread
            source_area = source[:, 3, None, :]
            kernel = source_area / (four_pi * jnp.sqrt(square + source_area))
            return (running + lax.optimization_barrier(jnp.sum(kernel * source[:, 4, None, :], axis=2)), None)
        nearby, _ = lax.scan(near_step, jnp.zeros((group, panels), jnp.float32), near_block.T)
        gathered = poles[far_block]
        segment_keys = (jnp.arange(group, dtype=jnp.int32)[:, None] * offsets + offset_block).reshape(-1)
        summed = jax.ops.segment_sum(gathered.reshape(-1, terms), segment_keys, num_segments=group * offsets)
        local = jnp.einsum('tok,oik->ti', summed.reshape(group, offsets, terms), table, precision=highest)
        return (nearby, local)
    nearby, local = lax.map(segment_work, (coords.reshape(-1, group, 3, panels), near_rows.reshape(-1, group, near_list.shape[1]), far_rows.reshape(-1, group, far_count), far_offset.reshape(-1, group, far_count)))
    nearby = nearby.reshape(leaves, panels)
    local = local.reshape(leaves, terms).astype(jnp.bfloat16)
    local = lax.optimization_barrier(local)
    distant = jnp.einsum('lpk,lk->lp', l2p.astype(jnp.float32), local.astype(jnp.float32), precision=highest)
    image = (0.5 * current + nearby + distant) * live_mask
    masked = basis * live_mask[None]
    population = jnp.sum(live_mask) * panels
    coefficients = jnp.einsum('jlp,lp->j', masked, image, precision=highest) / population
    residue = image - jnp.einsum('j,jlp->lp', coefficients, masked, precision=highest)
    scale = jnp.sqrt(jnp.sum(residue * residue) / population + epsilon)
    return (residue / scale, jnp.concatenate([coefficients, scale[None]]))
```

```python
import math

import jax
import jax.numpy as jnp
from jax import lax
from jax.experimental import pallas as pl
from jax.experimental.pallas import tpu as pltpu
from jax.sharding import Mesh
from jax.sharding import PartitionSpec as P

Y, Z, C, X = "seg_0", "seg_1", "seg_2", "grp"
AXES = (Y, Z, C, X)
MESH = pl.DeviceIdType.MESH
NT = (((1,), (1,)), ((), ()))
four_pi = 12.566370614359172
epsilon = 1e-06
f32 = jnp.float32
bf16 = jnp.bfloat16


def round_up(value, step):
    return -(-value // step) * step


def high_low(value):
    high = value.astype(bf16).astype(f32)
    return high, value - high


def two_parts(value):
    high, low = high_low(value)
    return high, low.astype(bf16).astype(f32)


def make_step(sizes, krylov, leaves, panels, terms, offsets, near, far):
    ny, nz, nc, nx = sizes
    segments = ny * nz * nc
    window = 3 * nx * leaves
    wide = round_up(window, 128)
    off_pad = round_up(offsets, 16)
    far_pad = round_up(far, 128)
    lanes = 128
    group_a = nx * nc
    group_b = ny * nz
    rows = 16

    def kernel(
        basis_ref, coords_ref, areas_ref, counts_ref, near_ref, far_ref, off_ref,
        p2m_hbm, l2p_hbm, m2l_hbm,
        vec_ref, hess_ref,
        p2m_v, l2p_v, m2l_v, panels_v, poles_v, far_v, off_v, count_v, sum_v, left_v,
        right_v, weight_v, part_v, near_v, stage_a, stage_b,
        load_sem, pole_send, pole_recv, panel_send, panel_recv, a_send, a_recv, b_send, b_recv,
    ):
        y, z, c, x = (lax.axis_index(name) for name in AXES)
        q = y * nz + z
        seg = q * nc + c
        q_across = lax.rem(q + group_b - 1 + 2 * c, group_b)
        y_across, z_across = q_across // nz, lax.rem(q_across, nz)

        loads = [
            pltpu.make_async_copy(src, dst, load_sem.at[k])
            for k, (src, dst) in enumerate(((p2m_hbm, p2m_v), (m2l_hbm, m2l_v), (l2p_hbm, l2p_v)))
        ]
        for load in loads:
            load.start()

        def ring(step):
            return lax.rem(x + step, nx)

        partner = (y, z, 1 - c, x)
        across = (y_across, z_across, 1 - c, x)
        peers_a = [(y, z, c, ring(r)) for r in range(1, nx)]
        peers_a += [(y, z, 1 - c, ring(r)) for r in range(nx)]
        peers_b = []
        for r in range(1, group_b):
            other = lax.rem(q + r, group_b)
            peers_b.append((other // nz, lax.rem(other, nz), c, x))

        barrier = pltpu.get_barrier_semaphore()
        everyone = peers_a + peers_b + [across]
        for peer in everyone:
            pl.semaphore_signal(barrier, inc=1, device_id=peer, device_id_type=MESH)

        slot_rows = lax.broadcasted_iota(jnp.int32, (leaves, panels), 0)
        mask = (slot_rows < counts_ref[0]).astype(f32)
        current = basis_ref[krylov - 1] * mask
        own = nx + x
        for comp in range(3):
            panels_v[own, comp] = coords_ref[:, comp, :]
        panels_v[own, 3] = areas_ref[...]
        panels_v[own, 4] = current

        padded = round_up(leaves, 16)

        def tall(value):
            extra = jnp.zeros((padded - leaves, value.shape[1]), f32)
            return jnp.concatenate([value, extra], axis=0).astype(bf16)

        rounded = tall(current)
        loads[0].wait()

        def to_poles(t, running):
            product = lax.dot_general(rounded, p2m_v[t], NT, preferred_element_type=f32)
            row = lax.broadcasted_iota(jnp.int32, product.shape, 0)
            return jnp.where(row == t, product, running)

        multipoles = lax.fori_loop(0, leaves, to_poles, jnp.zeros((padded, terms), f32))
        poles_v[own] = jnp.zeros((leaves, lanes), f32)
        poles_v[own, :, :terms] = multipoles[:leaves]

        pl.semaphore_wait(barrier, len(everyone))

        def send(buffer, sends, recvs, number, source, target_slot, peer):
            copy = pltpu.make_async_remote_copy(
                src_ref=buffer.at[source],
                dst_ref=buffer.at[target_slot],
                send_sem=sends.at[number],
                recv_sem=recvs.at[target_slot],
                device_id=peer,
                device_id_type=MESH,
            )
            copy.start()
            return copy

        sent = []

        def first_sends(buffer, sends, recvs):
            for r in range(1, nx):
                sent.append(send(buffer, sends, recvs, r - 1, own, own, (y, z, c, ring(r))))
            base = nx - 1
            sent.append(send(buffer, sends, recvs, base, own, 2 * nx * c + x, partner))
            sent.append(send(buffer, sends, recvs, base + 1, own, 2 * nx * (1 - c) + x, across))

        def received(buffer, sends, recvs, slot):
            pltpu.make_async_remote_copy(
                src_ref=buffer.at[slot],
                dst_ref=buffer.at[slot],
                send_sem=sends.at[0],
                recv_sem=recvs.at[slot],
                device_id=partner,
                device_id_type=MESH,
            ).wait_recv()

        def forward(buffer, sends, recvs, r):
            other = ring(r)
            received(buffer, sends, recvs, nx + other)
            base = nx + 1 + 2 * (r - 1)
            sent.append(send(buffer, sends, recvs, base, nx + other, 2 * nx * c + other, partner))
            sent.append(
                send(buffer, sends, recvs, base + 1, nx + other, 2 * nx * (1 - c) + other, across)
            )

        pole_set = (poles_v, pole_send, pole_recv)
        panel_set = (panels_v, panel_send, panel_recv)
        first_sends(*pole_set)
        first_sends(*panel_set)

        far_v[...] = jnp.full(far_v.shape, -1, jnp.int32)
        off_v[...] = jnp.full(off_v.shape, -1, jnp.int32)
        far_v[:, :far] = far_ref[...]
        off_v[:, :far] = off_ref[...]

        def to_counts(t, carry):
            off_row = jnp.broadcast_to(off_v[pl.ds(t, 1), :], (off_pad, far_pad))
            far_row = jnp.broadcast_to(far_v[pl.ds(t, 1), :], (wide, far_pad))
            off_hot = lax.broadcasted_iota(jnp.int32, (off_pad, far_pad), 0) == off_row
            far_hot = lax.broadcasted_iota(jnp.int32, (wide, far_pad), 0) == far_row
            pairs = lax.dot_general(
                jnp.where(off_hot, 1.0, 0.0).astype(bf16),
                jnp.where(far_hot, 1.0, 0.0).astype(bf16),
                NT,
                preferred_element_type=f32,
            )
            count_v[t] = pairs.astype(bf16)
            return carry

        lax.fori_loop(0, leaves, to_counts, 0)

        for r in (1, nx - 1, nx // 2):
            forward(*pole_set, r)

        left_v[...] = jnp.zeros(left_v.shape, bf16)
        own_comps = [panels_v[own, comp] - 2.0 for comp in range(3)]
        splits = [two_parts(value) for value in own_comps]
        norm = sum((value[0] + value[1]) * (value[0] + value[1]) for value in splits)
        norm_high, norm_low = high_low(norm)
        one = jnp.ones((leaves, panels), f32)
        zero = jnp.zeros((leaves, panels), f32)
        highs = [-2.0 * value[0] for value in splits]
        lows = [-2.0 * value[1] for value in splits]
        columns = highs + [one, one, one, norm_high, zero]
        columns += highs + [zero] * 5
        columns += lows + [zero, zero, zero, norm_low, zero]
        columns += lows + [zero] * 5
        for k, column in enumerate(columns):
            part_v[pl.ds(k, leaves, stride=2 * rows), :] = column

        def to_left(t, carry):
            block = part_v[pl.ds(pl.multiple_of(t * 2 * rows, 2 * rows), 2 * rows), :]
            left_v[t, :, : 2 * rows] = block.T.astype(bf16)
            return carry

        lax.fori_loop(0, leaves, to_left, 0)

        for r in (1, nx - 1, nx // 2):
            forward(*panel_set, r)

        tile_lane = lax.broadcasted_iota(jnp.int32, (krylov, lanes), 1)
        masked = [basis_ref[j] * mask for j in range(krylov)]

        def folded(value):
            return sum(value[8 * k : 8 * k + 8] for k in range(leaves // 8))

        def full_sum(value):
            return jnp.sum(jnp.sum(value, axis=0, keepdims=True), axis=1, keepdims=True)

        def inner_products(vector):
            lines = [
                jnp.sum(folded(masked[i] * vector), axis=0, keepdims=True) for i in range(krylov)
            ]
            return jnp.sum(jnp.concatenate(lines, axis=0), axis=1, keepdims=True)

        tile = jnp.zeros((krylov, lanes), f32)
        for j in range(krylov):
            tile = jnp.where(tile_lane == j, inner_products(masked[j]), tile)
        tile = jnp.where(tile_lane == krylov + 2, full_sum(folded(mask)), tile)

        valid_before = (seg > 0).astype(f32)
        valid_after = (seg < segments - 1).astype(f32)

        def outside_slots(recv):
            for k in range(nx):
                recv(k)
                recv(2 * nx + k)

        outside_slots(lambda slot: received(*pole_set, slot))

        pole_parts = []
        for slot in range(3 * nx):
            value = poles_v[slot]
            if slot < nx:
                value = value * valid_before
            if slot >= 2 * nx:
                value = value * valid_after
            pole_parts.append(value)
        pole_parts.append(jnp.zeros((wide - window, lanes), f32))
        all_poles = jnp.concatenate(pole_parts, axis=0)
        pole_high, pole_low = high_low(all_poles)
        both_poles = jnp.concatenate([pole_high, pole_low], axis=1).astype(bf16)

        def to_sums(t, carry):
            both = jnp.dot(count_v[t], both_poles, preferred_element_type=f32)
            start = pl.multiple_of(t * off_pad, off_pad)
            sum_v[pl.ds(start, off_pad), :] = both[:, :lanes] + both[:, lanes:]
            return carry

        lax.fori_loop(0, leaves, to_sums, 0)

        loads[1].wait()

        def to_local(o, running):
            sums = sum_v[pl.ds(o, leaves, stride=off_pad), :]
            high, low = high_low(sums)
            stacked = jnp.concatenate([high, low], axis=0).astype(bf16)
            return running + lax.dot_general(
                stacked[:, :terms], m2l_v[o], NT, preferred_element_type=f32
            )

        both = lax.fori_loop(
            0, offsets, to_local, jnp.zeros((2 * leaves, terms), f32), unroll=4
        )
        local = tall(both[:leaves] + both[leaves:])
        loads[2].wait()

        def to_distant(t, running):
            product = lax.dot_general(local, l2p_v[t], NT, preferred_element_type=f32)
            row = lax.broadcasted_iota(jnp.int32, product.shape, 0)
            return jnp.where(row == t, product, running)

        distant = lax.fori_loop(0, leaves, to_distant, jnp.zeros((padded, panels), f32))[:leaves]

        outside_slots(lambda slot: received(*panel_set, slot))

        for slot in range(3 * nx):
            parts = [two_parts(panels_v[slot, comp] - 2.0) for comp in range(3)]
            area = panels_v[slot, 3]
            weight = area * panels_v[slot, 4] * (1.0 / four_pi)
            if slot < nx:
                weight = weight * valid_before
            if slot >= 2 * nx:
                weight = weight * valid_after
            square = sum((value[0] + value[1]) * (value[0] + value[1]) for value in parts)
            first, rest = high_low(square + area)
            second, third = high_low(rest)
            lines = [value[0] for value in parts] + [first, second, third, one, zero]
            lines += [value[1] for value in parts] + [zero] * 5
            for k, line in enumerate(lines):
                right_v[slot * leaves : (slot + 1) * leaves, k, :] = line
            weight_v[slot * leaves : (slot + 1) * leaves, 0, :] = weight

        near_v[...] = jnp.zeros(near_v.shape, f32)
        pair_lane = lax.broadcasted_iota(jnp.int32, (panels, lanes), 1)

        def to_near(t, carry):
            left = left_v[t]
            running = jnp.zeros((panels, panels), f32)
            for start in range(0, near, 2):
                entries = [near_ref[t, n] for n in range(start, min(start + 2, near))]
                blocks = []
                for w in entries:
                    block = right_v[w].astype(bf16)
                    fill = jnp.zeros((lanes - 2 * rows, panels), bf16)
                    blocks.append(jnp.concatenate([block, block, fill], axis=0))
                right = jnp.concatenate(blocks, axis=1) if len(blocks) > 1 else blocks[0]
                square = jnp.dot(left, right, preferred_element_type=f32)
                for k, w in enumerate(entries):
                    inverse = lax.rsqrt(square[:, k * panels : (k + 1) * panels])
                    running = running + inverse * weight_v[w]
            total = jnp.sum(running, axis=1, keepdims=True)
            near_v[...] = jnp.where(pair_lane == t, total, near_v[...])
            return carry

        lax.fori_loop(0, leaves, to_near, 0)
        nearby = near_v[...].T[:leaves]

        image = (0.5 * current + nearby + distant) * mask
        tile = jnp.where(tile_lane == krylov, inner_products(image), tile)
        tile = jnp.where(tile_lane == krylov + 1, full_sum(folded(image * image)), tile)

        def exchange(stage, sends, recvs, me, others, value):
            stage[me] = value
            copies = []
            for k, (slot, peer) in enumerate(others):
                copy = pltpu.make_async_remote_copy(
                    src_ref=stage.at[me],
                    dst_ref=stage.at[me],
                    send_sem=sends.at[k],
                    recv_sem=recvs.at[me],
                    device_id=peer,
                    device_id_type=MESH,
                )
                copy.start()
                copies.append(copy)
            for slot, peer in others:
                pltpu.make_async_remote_copy(
                    src_ref=stage.at[slot],
                    dst_ref=stage.at[slot],
                    send_sem=sends.at[0],
                    recv_sem=recvs.at[slot],
                    device_id=peer,
                    device_id_type=MESH,
                ).wait_recv()
            total = stage[0]
            for k in range(1, stage.shape[0]):
                total = total + stage[k]
            sent.extend(copies)
            return total

        others_a = [(ring(r) * nc + c, (y, z, c, ring(r))) for r in range(1, nx)]
        others_a += [(ring(r) * nc + 1 - c, (y, z, 1 - c, ring(r))) for r in range(nx)]
        tile = exchange(stage_a, a_send, a_recv, x * nc + c, others_a, tile)
        others_b = [(lax.rem(q + r, group_b), peers_b[r - 1]) for r in range(1, group_b)]
        tile = exchange(stage_b, b_send, b_recv, q, others_b, tile)

        def column(index):
            return jnp.sum(jnp.where(tile_lane == index, tile, 0.0), axis=1, keepdims=True)

        population = column(krylov + 2)[:1]
        products = column(krylov)
        energy = column(krylov + 1)[:1]
        coefficients = products / population
        tile_row = lax.broadcasted_iota(jnp.int32, (krylov, lanes), 0)
        spread = jnp.sum(
            jnp.where(tile_lane == tile_row, coefficients, 0.0), axis=0, keepdims=True
        )
        gram = jnp.where(tile_lane < krylov, tile, 0.0)
        curvature = full_sum(gram * coefficients * spread)
        squares = energy - 2.0 * full_sum(coefficients * products) + curvature
        scale = jnp.sqrt(squares / population + epsilon)
        residue = image
        for j in range(krylov):
            residue = residue - coefficients[j : j + 1] * masked[j]
        vec_ref[...] = residue / scale
        lane_row = lax.broadcasted_iota(jnp.int32, (1, lanes), 1)
        hess_ref[...] = jnp.where(lane_row == krylov, scale, spread)

        for copy in sent:
            copy.wait_send()

    vmem = pl.BlockSpec(memory_space=pltpu.VMEM)
    smem = pl.BlockSpec(memory_space=pltpu.SMEM)
    anywhere = pl.BlockSpec(memory_space=pl.ANY)
    dma = pltpu.SemaphoreType.DMA
    slots = 3 * nx
    n_sends = nx + 1 + 2 * (nx - 1)
    return pl.pallas_call(
        kernel,
        out_shape=(
            jax.ShapeDtypeStruct((leaves, panels), f32),
            jax.ShapeDtypeStruct((1, lanes), f32),
        ),
        in_specs=[vmem, vmem, vmem, smem, smem, vmem, vmem, anywhere, anywhere, anywhere],
        out_specs=(vmem, vmem),
        scratch_shapes=[
            pltpu.VMEM((leaves, terms, panels), bf16),
            pltpu.VMEM((leaves, panels, terms), bf16),
            pltpu.VMEM((offsets, terms, terms), bf16),
            pltpu.VMEM((slots, 5, leaves, panels), f32),
            pltpu.VMEM((slots, leaves, lanes), f32),
            pltpu.VMEM((leaves, far_pad), jnp.int32),
            pltpu.VMEM((leaves, far_pad), jnp.int32),
            pltpu.VMEM((leaves, off_pad, wide), bf16),
            pltpu.VMEM((leaves * off_pad, lanes), f32),
            pltpu.VMEM((leaves, panels, lanes), bf16),
            pltpu.VMEM((window, rows, panels), f32),
            pltpu.VMEM((window, 1, panels), f32),
            pltpu.VMEM((leaves * 2 * rows, panels), f32),
            pltpu.VMEM((panels, lanes), f32),
            pltpu.VMEM((group_a, krylov, lanes), f32),
            pltpu.VMEM((group_b, krylov, lanes), f32),
            dma((3,)),
            dma((n_sends,)),
            dma((slots,)),
            dma((n_sends,)),
            dma((slots,)),
            dma((group_a,)),
            dma((group_a,)),
            dma((group_b,)),
            dma((group_b,)),
        ],
        compiler_params=pltpu.CompilerParams(
            collective_id=0, has_side_effects=True, vmem_limit_bytes=56 * 1024 * 1024
        ),
    )


def solution(mesh):
    torus = Mesh(mesh.devices.reshape(4, 4, 2, mesh.shape["grp"]), AXES)
    every = AXES

    def on_device(basis, coords, areas, p2m, l2p, m2l, counts, near_list, far_list, far_offset):
        krylov, leaves, panels = basis.shape
        step = make_step(
            torus.devices.shape, krylov, leaves, panels, p2m.shape[1], m2l.shape[0],
            near_list.shape[1], far_list.shape[1],
        )
        vector, hessenberg = step(
            basis, coords, areas, counts, near_list, far_list, far_offset, p2m, l2p, m2l
        )
        return vector, hessenberg[0, : krylov + 1]

    in_specs = (
        P(None, every, None),
        P(every, None, None),
        P(every, None),
        P(every, None, None),
        P(every, None, None),
        P(),
        P(every),
        P(every, None),
        P(every, None),
        P(every, None),
    )
    out_specs = (P(every, None), P())
    return jax.shard_map(
        on_device, mesh=torus, in_specs=in_specs, out_specs=out_specs, check_vma=False
    )
```

```python
import math

import jax
import jax.numpy as jnp
from jax import lax
from jax.experimental import pallas as pl
from jax.experimental.pallas import tpu as pltpu
from jax.sharding import Mesh
from jax.sharding import PartitionSpec as P

Y, Z, C, X = "seg_0", "seg_1", "seg_2", "grp"
AXES = (Y, Z, C, X)
MESH = pl.DeviceIdType.MESH
NT = (((1,), (1,)), ((), ()))
four_pi = 12.566370614359172
epsilon = 1e-06
f32 = jnp.float32
bf16 = jnp.bfloat16


def round_up(value, step):
    return -(-value // step) * step


def high_low(value):
    high = value.astype(bf16).astype(f32)
    return high, value - high


def two_parts(value):
    high, low = high_low(value)
    return high, low.astype(bf16).astype(f32)


def make_step(sizes, krylov, leaves, panels, terms, offsets, near, far):
    ny, nz, nc, nx = sizes
    segments = ny * nz * nc
    window = 3 * nx * leaves
    wide = round_up(window, 128)
    off_pad = round_up(offsets, 16)
    off_step = off_pad + 8
    far_pad = round_up(far, 128)
    lanes = 128
    group_a = nx * nc
    group_b = ny * nz
    rows = 16
    row_step = 24
    part_step = 40
    group = 8
    folded_rows = group * lanes

    def kernel(
        basis_ref, coords_ref, areas_ref, counts_ref, near_ref, far_ref, off_ref,
        p2m_hbm, l2p_hbm, m2l_hbm,
        vec_ref, hess_ref,
        p2m_v, l2p_v, m2l_v, panels_v, poles_v, far_v, off_v, count_v, sum_v, left_v,
        right_v, part_v, near_v, p2m_f, l2p_f, m2l_f, stage_a, stage_b,
        load_sem, pole_send, pole_recv, panel_send, panel_recv, a_send, a_recv, b_send, b_recv,
    ):
        y, z, c, x = (lax.axis_index(name) for name in AXES)
        q = y * nz + z
        seg = q * nc + c
        q_across = lax.rem(q + group_b - 1 + 2 * c, group_b)
        y_across, z_across = q_across // nz, lax.rem(q_across, nz)

        loads = [
            pltpu.make_async_copy(src, dst, load_sem.at[k])
            for k, (src, dst) in enumerate(((p2m_hbm, p2m_v), (m2l_hbm, m2l_v), (l2p_hbm, l2p_v)))
        ]
        for load in loads:
            load.start()

        def ring(step):
            return lax.rem(x + step, nx)

        partner = (y, z, 1 - c, x)
        across = (y_across, z_across, 1 - c, x)
        peers_a = [(y, z, c, ring(r)) for r in range(1, nx)]
        peers_a += [(y, z, 1 - c, ring(r)) for r in range(nx)]
        peers_b = []
        for r in range(1, group_b):
            other = lax.rem(q + r, group_b)
            peers_b.append((other // nz, lax.rem(other, nz), c, x))

        barrier = pltpu.get_barrier_semaphore()
        everyone = peers_a + peers_b + [across]
        for peer in everyone:
            pl.semaphore_signal(barrier, inc=1, device_id=peer, device_id_type=MESH)

        slot_rows = lax.broadcasted_iota(jnp.int32, (leaves, panels), 0)
        mask = (slot_rows < counts_ref[0]).astype(f32)
        current = basis_ref[krylov - 1] * mask
        own = nx + x
        for comp in range(3):
            panels_v[own, comp] = coords_ref[comp]
        panels_v[own, 3] = areas_ref[...]
        panels_v[own, 4] = current

        padded = round_up(leaves, 16)

        def tall(value):
            extra = jnp.zeros((padded - leaves, value.shape[1]), f32)
            return jnp.concatenate([value, extra], axis=0).astype(bf16)

        rounded = tall(current)
        loads[0].wait()

        def unfold(source, scratch, part, count):
            block = source[:, pl.ds(pl.multiple_of(part * group, group), count), :].astype(f32)
            width = block.shape[2]
            if count == group:
                scratch[: block.shape[0] * group, :width] = block.reshape(-1, width)
            else:
                for k in range(block.shape[0]):
                    scratch[k * group : k * group + count, :width] = block[k]

        def unfolded(scratch, k):
            return scratch[pl.ds(k, lanes, stride=group), :].astype(bf16)

        def per_leaf(values, source, scratch, dims, running):
            def one_group(part, running):
                unfold(source, scratch, part, group)
                for k in range(group):
                    product = lax.dot_general(
                        values, unfolded(scratch, k), dims, preferred_element_type=f32
                    )
                    row = lax.broadcasted_iota(jnp.int32, product.shape, 0)
                    running = jnp.where(row == part * group + k, product, running)
                return running

            return lax.fori_loop(0, leaves // group, one_group, running)

        blank = jnp.zeros((padded, lanes), f32)
        multipoles = per_leaf(rounded, p2m_v, p2m_f, NT, blank)
        poles_v[own] = jnp.zeros((leaves, lanes), f32)
        poles_v[own, :, :terms] = multipoles[:leaves, :terms]

        pattern = (lax.broadcasted_iota(jnp.int32, (window, rows, panels), 1) == 6).astype(f32)
        right_v[:, :rows, :] = pattern
        for scratch in (l2p_f, m2l_f):
            scratch[...] = jnp.zeros(scratch.shape, f32)

        pl.semaphore_wait(barrier, len(everyone))

        def send(buffer, sends, recvs, number, source, target_slot, peer):
            copy = pltpu.make_async_remote_copy(
                src_ref=buffer.at[source],
                dst_ref=buffer.at[target_slot],
                send_sem=sends.at[number],
                recv_sem=recvs.at[target_slot],
                device_id=peer,
                device_id_type=MESH,
            )
            copy.start()
            return copy

        sent = []

        def first_sends(buffer, sends, recvs):
            for r in range(1, nx):
                sent.append(send(buffer, sends, recvs, r - 1, own, own, (y, z, c, ring(r))))
            base = nx - 1
            sent.append(send(buffer, sends, recvs, base, own, 2 * nx * c + x, partner))
            sent.append(send(buffer, sends, recvs, base + 1, own, 2 * nx * (1 - c) + x, across))

        def received(buffer, sends, recvs, slot):
            pltpu.make_async_remote_copy(
                src_ref=buffer.at[slot],
                dst_ref=buffer.at[slot],
                send_sem=sends.at[0],
                recv_sem=recvs.at[slot],
                device_id=partner,
                device_id_type=MESH,
            ).wait_recv()

        def forward(buffer, sends, recvs, r):
            other = ring(r)
            received(buffer, sends, recvs, nx + other)
            base = nx + 1 + 2 * (r - 1)
            sent.append(send(buffer, sends, recvs, base, nx + other, 2 * nx * c + other, partner))
            sent.append(
                send(buffer, sends, recvs, base + 1, nx + other, 2 * nx * (1 - c) + other, across)
            )

        pole_set = (poles_v, pole_send, pole_recv)
        panel_set = (panels_v, panel_send, panel_recv)
        first_sends(*pole_set)
        first_sends(*panel_set)

        far_v[...] = jnp.full(far_v.shape, -1, jnp.int32)
        off_v[...] = jnp.full(off_v.shape, -1, jnp.int32)
        far_v[:, :far] = far_ref[...]
        off_v[:, :far] = off_ref[...]

        def to_counts(t, carry):
            off_row = jnp.broadcast_to(off_v[pl.ds(t, 1), :], (off_pad, far_pad))
            far_row = jnp.broadcast_to(far_v[pl.ds(t, 1), :], (wide, far_pad))
            off_hot = lax.broadcasted_iota(jnp.int32, (off_pad, far_pad), 0) == off_row
            far_hot = lax.broadcasted_iota(jnp.int32, (wide, far_pad), 0) == far_row
            pairs = lax.dot_general(
                jnp.where(off_hot, 1.0, 0.0).astype(bf16),
                jnp.where(far_hot, 1.0, 0.0).astype(bf16),
                NT,
                preferred_element_type=f32,
            )
            count_v[t] = pairs.astype(bf16)
            return carry

        third = leaves // 4
        lax.fori_loop(0, 2 * third, to_counts, 0, unroll=2)
        forward(*pole_set, 1)
        forward(*pole_set, nx - 1)
        lax.fori_loop(2 * third, 3 * third, to_counts, 0, unroll=2)
        forward(*pole_set, nx // 2)
        forward(*panel_set, 1)
        forward(*panel_set, nx - 1)
        lax.fori_loop(3 * third, leaves, to_counts, 0, unroll=2)

        left_v[...] = jnp.zeros(left_v.shape, bf16)
        own_comps = [panels_v[own, comp] - 2.0 for comp in range(3)]
        splits = [two_parts(value) for value in own_comps]
        norm = sum((value[0] + value[1]) * (value[0] + value[1]) for value in splits)
        norm_high, norm_low = high_low(norm)
        one = jnp.ones((leaves, panels), f32)
        zero = jnp.zeros((leaves, panels), f32)
        highs = [-2.0 * value[0] for value in splits]
        lows = [-2.0 * value[1] for value in splits]
        columns = highs + [one, one, one, norm_high, zero]
        columns += highs + [zero] * 5
        columns += lows + [zero, zero, zero, norm_low, zero]
        columns += lows + [zero] * 5
        for k, column in enumerate(columns):
            part_v[pl.ds(k, leaves, stride=part_step), :] = column

        def to_left(t, carry):
            block = part_v[pl.ds(pl.multiple_of(t * part_step, 8), 2 * rows), :]
            left_v[t, :, : 2 * rows] = block.T.astype(bf16)
            return carry

        lax.fori_loop(0, leaves, to_left, 0, unroll=4)
        forward(*panel_set, nx // 2)

        tile_lane = lax.broadcasted_iota(jnp.int32, (krylov, lanes), 1)
        masked = [basis_ref[j] * mask for j in range(krylov)]

        def folded(value):
            return sum(value[8 * k : 8 * k + 8] for k in range(leaves // 8))

        def full_sum(value):
            return jnp.sum(jnp.sum(value, axis=0, keepdims=True), axis=1, keepdims=True)

        def inner_products(vector):
            lines = [
                jnp.sum(folded(masked[i] * vector), axis=0, keepdims=True) for i in range(krylov)
            ]
            return jnp.sum(jnp.concatenate(lines, axis=0), axis=1, keepdims=True)

        tile = jnp.zeros((krylov, lanes), f32)
        for j in range(krylov):
            tile = jnp.where(tile_lane == j, inner_products(masked[j]), tile)
        tile = jnp.where(tile_lane == krylov + 2, full_sum(folded(mask)), tile)

        valid_before = (seg > 0).astype(f32)
        valid_after = (seg < segments - 1).astype(f32)

        def outside_slots(recv):
            for k in range(nx):
                recv(k)
                recv(2 * nx + k)

        outside_slots(lambda slot: received(*pole_set, slot))

        pole_parts = []
        for slot in range(3 * nx):
            value = poles_v[slot]
            if slot < nx:
                value = value * valid_before
            if slot >= 2 * nx:
                value = value * valid_after
            pole_parts.append(value)
        pole_parts.append(jnp.zeros((wide - window, lanes), f32))
        all_poles = jnp.concatenate(pole_parts, axis=0)
        pole_high, pole_low = high_low(all_poles)
        both_poles = jnp.concatenate([pole_high, pole_low], axis=1).astype(bf16)

        def to_sums(t, carry):
            both = jnp.dot(count_v[t], both_poles, preferred_element_type=f32)
            start = pl.multiple_of(t * off_step, 8)
            sum_v[pl.ds(start, off_pad), :] = both[:, :lanes] + both[:, lanes:]
            return carry

        lax.fori_loop(0, leaves, to_sums, 0, unroll=2)

        loads[1].wait()

        def add_local(part, half, count, running):
            scratch = m2l_f.at[half]
            unfold(m2l_v, scratch, part, count)
            for k in range(0, count, 2):
                lefts, rights = [], []
                for o in (k, k + 1):
                    sums = sum_v[pl.ds(part * group + o, leaves, stride=off_step), :]
                    high, low = high_low(sums)
                    lefts.append(jnp.concatenate([high, low], axis=0).astype(bf16))
                    rights.append(unfolded(scratch, o))
                running = running + lax.dot_general(
                    jnp.concatenate(lefts, axis=1),
                    jnp.concatenate(rights, axis=1),
                    NT,
                    preferred_element_type=f32,
                )
            return running

        def to_local(step, running):
            for half in range(2):
                running = add_local(2 * step + half, half, group, running)
            return running

        whole = offsets // group
        both = lax.fori_loop(0, whole // 2, to_local, jnp.zeros((2 * leaves, lanes), f32))
        for part in range(whole // 2 * 2, whole):
            both = add_local(part, 0, group, both)
        if offsets % group:
            both = add_local(whole, 1, offsets % group, both)
        inside = lax.broadcasted_iota(jnp.int32, (leaves, lanes), 1) < terms
        local = tall(jnp.where(inside, both[:leaves] + both[leaves:], 0.0))
        loads[2].wait()
        plain = (((1,), (0,)), ((), ()))
        distant = per_leaf(local, l2p_v, l2p_f, plain, blank)[:leaves]

        outside_slots(lambda slot: received(*panel_set, slot))

        for slot in range(3 * nx):
            parts = [two_parts(panels_v[slot, comp] - 2.0) for comp in range(3)]
            area = panels_v[slot, 3]
            weight = area * panels_v[slot, 4] * (1.0 / four_pi)
            if slot < nx:
                weight = weight * valid_before
            if slot >= 2 * nx:
                weight = weight * valid_after
            square = sum((value[0] + value[1]) * (value[0] + value[1]) for value in parts)
            first, rest = high_low(square + area)
            second, third = high_low(rest)
            lines = [value[0] for value in parts] + [first, second, third]
            lines = list(enumerate(lines)) + [(7, weight)]
            lines += [(8 + k, value[1]) for k, value in enumerate(parts)]
            flat = right_v.reshape(window * row_step, panels)
            for k, line in lines:
                flat[pl.ds(slot * leaves * row_step + k, leaves, stride=row_step), :] = line

        near_v[...] = jnp.zeros(near_v.shape, f32)
        pair_lane = lax.broadcasted_iota(jnp.int32, (panels, lanes), 1)

        def to_near(t, carry):
            left = left_v[t]
            running = jnp.zeros((panels, panels), f32)
            for start in range(0, near, 2):
                entries = [near_ref[t, n] for n in range(start, min(start + 2, near))]
                blocks = []
                for w in entries:
                    block = right_v[w, :rows, :].astype(bf16)
                    fill = jnp.zeros((lanes - 2 * rows, panels), bf16)
                    blocks.append(jnp.concatenate([block, block, fill], axis=0))
                right = jnp.concatenate(blocks, axis=1) if len(blocks) > 1 else blocks[0]
                square = jnp.dot(left, right, preferred_element_type=f32)
                for k, w in enumerate(entries):
                    inverse = lax.rsqrt(square[:, k * panels : (k + 1) * panels])
                    running = running + inverse * right_v[w, 7:8, :]
            total = jnp.sum(running, axis=1, keepdims=True)
            near_v[...] = jnp.where(pair_lane == t, total, near_v[...])
            return carry

        lax.fori_loop(0, leaves, to_near, 0, unroll=8)
        nearby = near_v[...].T[:leaves]

        image = (0.5 * current + nearby + distant) * mask
        tile = jnp.where(tile_lane == krylov, inner_products(image), tile)
        tile = jnp.where(tile_lane == krylov + 1, full_sum(folded(image * image)), tile)

        def exchange(stage, sends, recvs, me, others, value):
            stage[me] = value
            copies = []
            for k, (slot, peer) in enumerate(others):
                copy = pltpu.make_async_remote_copy(
                    src_ref=stage.at[me],
                    dst_ref=stage.at[me],
                    send_sem=sends.at[k],
                    recv_sem=recvs.at[me],
                    device_id=peer,
                    device_id_type=MESH,
                )
                copy.start()
                copies.append(copy)
            for slot, peer in others:
                pltpu.make_async_remote_copy(
                    src_ref=stage.at[slot],
                    dst_ref=stage.at[slot],
                    send_sem=sends.at[0],
                    recv_sem=recvs.at[slot],
                    device_id=peer,
                    device_id_type=MESH,
                ).wait_recv()
            total = stage[0]
            for k in range(1, stage.shape[0]):
                total = total + stage[k]
            sent.extend(copies)
            return total

        others_a = [(ring(r) * nc + c, (y, z, c, ring(r))) for r in range(1, nx)]
        others_a += [(ring(r) * nc + 1 - c, (y, z, 1 - c, ring(r))) for r in range(nx)]
        tile = exchange(stage_a, a_send, a_recv, x * nc + c, others_a, tile)
        others_b = [(lax.rem(q + r, group_b), peers_b[r - 1]) for r in range(1, group_b)]
        tile = exchange(stage_b, b_send, b_recv, q, others_b, tile)

        def column(index):
            return jnp.sum(jnp.where(tile_lane == index, tile, 0.0), axis=1, keepdims=True)

        population = column(krylov + 2)[:1]
        products = column(krylov)
        energy = column(krylov + 1)[:1]
        coefficients = products / population
        tile_row = lax.broadcasted_iota(jnp.int32, (krylov, lanes), 0)
        spread = jnp.sum(
            jnp.where(tile_lane == tile_row, coefficients, 0.0), axis=0, keepdims=True
        )
        gram = jnp.where(tile_lane < krylov, tile, 0.0)
        curvature = full_sum(gram * coefficients * spread)
        squares = energy - 2.0 * full_sum(coefficients * products) + curvature
        scale = jnp.sqrt(squares / population + epsilon)
        residue = image
        for j in range(krylov):
            residue = residue - coefficients[j : j + 1] * masked[j]
        vec_ref[...] = residue / scale
        lane_row = lax.broadcasted_iota(jnp.int32, (1, lanes), 1)
        hess_ref[...] = jnp.where(lane_row == krylov, scale, spread)

        for copy in sent:
            copy.wait_send()

    vmem = pl.BlockSpec(memory_space=pltpu.VMEM)
    smem = pl.BlockSpec(memory_space=pltpu.SMEM)
    anywhere = pl.BlockSpec(memory_space=pl.ANY)
    dma = pltpu.SemaphoreType.DMA
    slots = 3 * nx
    n_sends = nx + 1 + 2 * (nx - 1)
    return pl.pallas_call(
        kernel,
        out_shape=(
            jax.ShapeDtypeStruct((leaves, panels), f32),
            jax.ShapeDtypeStruct((1, lanes), f32),
        ),
        in_specs=[vmem, vmem, vmem, smem, smem, vmem, vmem, anywhere, anywhere, anywhere],
        out_specs=(vmem, vmem),
        scratch_shapes=[
            pltpu.VMEM((terms, leaves, panels), bf16),
            pltpu.VMEM((terms, leaves, panels), bf16),
            pltpu.VMEM((terms, offsets, terms), bf16),
            pltpu.VMEM((slots, 5, leaves, panels), f32),
            pltpu.VMEM((slots, leaves, lanes), f32),
            pltpu.VMEM((leaves, far_pad), jnp.int32),
            pltpu.VMEM((leaves, far_pad), jnp.int32),
            pltpu.VMEM((leaves, off_pad, wide), bf16),
            pltpu.VMEM((leaves * off_step, lanes), f32),
            pltpu.VMEM((leaves, panels, lanes), bf16),
            pltpu.VMEM((window, row_step, panels), f32),
            pltpu.VMEM((leaves * part_step, panels), f32),
            pltpu.VMEM((panels, lanes), f32),
            pltpu.VMEM((folded_rows, lanes), f32),
            pltpu.VMEM((folded_rows, lanes), f32),
            pltpu.VMEM((2, folded_rows, lanes), f32),
            pltpu.VMEM((group_a, krylov, lanes), f32),
            pltpu.VMEM((group_b, krylov, lanes), f32),
            dma((3,)),
            dma((n_sends,)),
            dma((slots,)),
            dma((n_sends,)),
            dma((slots,)),
            dma((group_a,)),
            dma((group_a,)),
            dma((group_b,)),
            dma((group_b,)),
        ],
        compiler_params=pltpu.CompilerParams(
            collective_id=0, has_side_effects=True, vmem_limit_bytes=56 * 1024 * 1024
        ),
    )


def solution(mesh):
    torus = Mesh(mesh.devices.reshape(4, 4, 2, mesh.shape["grp"]), AXES)
    every = AXES

    def on_device(basis, coords, areas, p2m, l2p, m2l, counts, near_list, far_list, far_offset):
        krylov, leaves, panels = basis.shape
        step = make_step(
            torus.devices.shape, krylov, leaves, panels, p2m.shape[1], m2l.shape[0],
            near_list.shape[1], far_list.shape[1],
        )
        vector, hessenberg = step(
            basis, coords.transpose(1, 0, 2), areas, counts, near_list, far_list, far_offset,
            p2m.transpose(1, 0, 2), l2p.transpose(2, 0, 1), m2l.transpose(1, 0, 2),
        )
        return vector, hessenberg[0, : krylov + 1]

    in_specs = (
        P(None, every, None),
        P(every, None, None),
        P(every, None),
        P(every, None, None),
        P(every, None, None),
        P(),
        P(every),
        P(every, None),
        P(every, None),
        P(every, None),
    )
    out_specs = (P(every, None), P())
    return jax.shard_map(
        on_device, mesh=torus, in_specs=in_specs, out_specs=out_specs, check_vma=False
    )
```

```python
import math

import jax
import jax.numpy as jnp
from jax import lax
from jax.experimental import pallas as pl
from jax.experimental.pallas import tpu as pltpu
from jax.sharding import Mesh
from jax.sharding import PartitionSpec as P

Y, Z, C, X = "seg_0", "seg_1", "seg_2", "grp"
AXES = (Y, Z, C, X)
MESH = pl.DeviceIdType.MESH
NT = (((1,), (1,)), ((), ()))
four_pi = 12.566370614359172
epsilon = 1e-06
f32 = jnp.float32
bf16 = jnp.bfloat16


def round_up(value, step):
    return -(-value // step) * step


def high_low(value):
    high = value.astype(bf16).astype(f32)
    return high, value - high


def two_parts(value):
    high, low = high_low(value)
    return high, low.astype(bf16).astype(f32)


def make_step(sizes, krylov, leaves, panels, terms, offsets, near, far):
    ny, nz, nc, nx = sizes
    segments = ny * nz * nc
    window = 3 * nx * leaves
    wide = round_up(window, 128)
    off_pad = round_up(offsets, 16)
    off_step = off_pad + 4
    far_pad = round_up(far, 128)
    lanes = 128
    group_a = nx * nc
    group_b = ny * nz
    rows = 16
    row_step = 24
    part_step = 40
    group = 8
    leaf_step = group + 1
    folded_rows = round_up((lanes - 1) * leaf_step + group, 8)
    buffers = 4

    def kernel(
        basis_ref, coords_ref, areas_ref, counts_ref, near_ref, far_ref, off_ref,
        p2m_hbm, l2p_hbm, m2l_hbm,
        vec_ref, hess_ref,
        p2m_v, l2p_v, m2l_v, panels_v, poles_v, far_v, off_v, count_v, sum_v, left_v,
        right_v, part_v, near_v, p2m_f, l2p_f, m2l_f, pair_v, stage_a, stage_b,
        load_sem, pole_send, pole_recv, panel_send, panel_recv, a_send, a_recv, b_send, b_recv,
    ):
        y, z, c, x = (lax.axis_index(name) for name in AXES)
        q = y * nz + z
        seg = q * nc + c
        q_across = lax.rem(q + group_b - 1 + 2 * c, group_b)
        y_across, z_across = q_across // nz, lax.rem(q_across, nz)

        loads = [
            pltpu.make_async_copy(src, dst, load_sem.at[k])
            for k, (src, dst) in enumerate(((p2m_hbm, p2m_v), (m2l_hbm, m2l_v), (l2p_hbm, l2p_v)))
        ]
        for load in loads:
            load.start()

        def ring(step):
            return lax.rem(x + step, nx)

        partner = (y, z, 1 - c, x)
        across = (y_across, z_across, 1 - c, x)
        peers_a = [(y, z, c, ring(r)) for r in range(1, nx)]
        peers_a += [(y, z, 1 - c, ring(r)) for r in range(nx)]
        peers_b = []
        for r in range(1, group_b):
            other = lax.rem(q + r, group_b)
            peers_b.append((other // nz, lax.rem(other, nz), c, x))

        barrier = pltpu.get_barrier_semaphore()
        everyone = peers_a + peers_b + [across]
        for peer in everyone:
            pl.semaphore_signal(barrier, inc=1, device_id=peer, device_id_type=MESH)

        slot_rows = lax.broadcasted_iota(jnp.int32, (leaves, panels), 0)
        mask = (slot_rows < counts_ref[0]).astype(f32)
        current = basis_ref[krylov - 1] * mask
        own = nx + x
        for comp in range(3):
            panels_v[own, comp] = coords_ref[comp]
        panels_v[own, 3] = areas_ref[...]
        panels_v[own, 4] = current

        padded = round_up(leaves, 16)

        def tall(value):
            extra = jnp.zeros((padded - leaves, value.shape[1]), f32)
            return jnp.concatenate([value, extra], axis=0).astype(bf16)

        rounded = tall(current)
        loads[0].wait()

        def unfold(source, scratch, part, count):
            start = part * group
            if not isinstance(part, int):
                start = pl.multiple_of(start, group)
            block = source[:, pl.ds(start, count), :].astype(f32)
            width = block.shape[2]
            for k in range(block.shape[0]):
                scratch[k * leaf_step : k * leaf_step + count, :width] = block[k]

        def unfolded(scratch, k):
            return scratch[pl.ds(k, lanes, stride=leaf_step), :].astype(bf16)

        def per_leaf(values, source, scratch, dims, running):
            def one_group(part, running):
                unfold(source, scratch, part, group)
                for k in range(group):
                    product = lax.dot_general(
                        values, unfolded(scratch, k), dims, preferred_element_type=f32
                    )
                    row = lax.broadcasted_iota(jnp.int32, product.shape, 0)
                    running = jnp.where(row == part * group + k, product, running)
                return running

            return lax.fori_loop(0, leaves // group, one_group, running)

        blank = jnp.zeros((padded, lanes), f32)
        multipoles = per_leaf(rounded, p2m_v, p2m_f, NT, blank)
        poles_v[own] = jnp.zeros((leaves, lanes), f32)
        poles_v[own, :, :terms] = multipoles[:leaves, :terms]

        pattern = (lax.broadcasted_iota(jnp.int32, (window, rows, panels), 1) == 6).astype(f32)
        right_v[:, :rows, :] = pattern
        for scratch in (l2p_f, m2l_f):
            scratch[...] = jnp.zeros(scratch.shape, f32)

        far_v[...] = jnp.full(far_v.shape, -1, jnp.int32)
        off_v[...] = jnp.full(off_v.shape, -1, jnp.int32)
        far_v[:, :far] = far_ref[...]
        off_v[:, :far] = off_ref[...]

        def to_counts(t, carry):
            off_row = jnp.broadcast_to(off_v[pl.ds(t, 1), :], (off_pad, far_pad))
            far_row = jnp.broadcast_to(far_v[pl.ds(t, 1), :], (wide, far_pad))
            off_hot = lax.broadcasted_iota(jnp.int32, (off_pad, far_pad), 0) == off_row
            far_hot = lax.broadcasted_iota(jnp.int32, (wide, far_pad), 0) == far_row
            pairs = lax.dot_general(
                jnp.where(off_hot, 1.0, 0.0).astype(bf16),
                jnp.where(far_hot, 1.0, 0.0).astype(bf16),
                NT,
                preferred_element_type=f32,
            )
            count_v[t] = pairs.astype(bf16)
            return carry

        lax.fori_loop(0, leaves, to_counts, 0, unroll=4)

        left_v[...] = jnp.zeros(left_v.shape, bf16)
        own_comps = [panels_v[own, comp] - 2.0 for comp in range(3)]
        splits = [two_parts(value) for value in own_comps]
        norm = sum((value[0] + value[1]) * (value[0] + value[1]) for value in splits)
        norm_high, norm_low = high_low(norm)
        one = jnp.ones((leaves, panels), f32)
        zero = jnp.zeros((leaves, panels), f32)
        highs = [-2.0 * value[0] for value in splits]
        lows = [-2.0 * value[1] for value in splits]
        columns = highs + [one, one, one, norm_high, zero]
        columns += highs + [zero] * 5
        columns += lows + [zero, zero, zero, norm_low, zero]
        columns += lows + [zero] * 5
        for k, column in enumerate(columns):
            part_v[pl.ds(k, leaves, stride=part_step), :] = column

        def to_left(t, carry):
            block = part_v[pl.ds(pl.multiple_of(t * part_step, 8), 2 * rows), :]
            left_v[t, :, : 2 * rows] = block.T.astype(bf16)
            return carry

        lax.fori_loop(0, leaves, to_left, 0, unroll=4)
        tile_lane = lax.broadcasted_iota(jnp.int32, (krylov, lanes), 1)
        masked = [basis_ref[j] * mask for j in range(krylov)]

        def folded(value):
            return sum(value[8 * k : 8 * k + 8] for k in range(leaves // 8))

        def full_sum(value):
            return jnp.sum(jnp.sum(value, axis=0, keepdims=True), axis=1, keepdims=True)

        def inner_products(vector):
            lines = [
                jnp.sum(folded(masked[i] * vector), axis=0, keepdims=True) for i in range(krylov)
            ]
            return jnp.sum(jnp.concatenate(lines, axis=0), axis=1, keepdims=True)

        tile = jnp.zeros((krylov, lanes), f32)
        for j in range(krylov):
            tile = jnp.where(tile_lane == j, inner_products(masked[j]), tile)
        tile = jnp.where(tile_lane == krylov + 2, full_sum(folded(mask)), tile)

        pl.semaphore_wait(barrier, len(everyone))

        def send(buffer, sends, recvs, number, source, target_slot, peer):
            copy = pltpu.make_async_remote_copy(
                src_ref=buffer.at[source],
                dst_ref=buffer.at[target_slot],
                send_sem=sends.at[number],
                recv_sem=recvs.at[target_slot],
                device_id=peer,
                device_id_type=MESH,
            )
            copy.start()
            return copy

        sent = []

        def first_sends(buffer, sends, recvs):
            for r in range(1, nx):
                sent.append(send(buffer, sends, recvs, r - 1, own, own, (y, z, c, ring(r))))
            base = nx - 1
            sent.append(send(buffer, sends, recvs, base, own, 2 * nx * c + x, partner))
            sent.append(send(buffer, sends, recvs, base + 1, own, 2 * nx * (1 - c) + x, across))

        def received(buffer, sends, recvs, slot):
            pltpu.make_async_remote_copy(
                src_ref=buffer.at[slot],
                dst_ref=buffer.at[slot],
                send_sem=sends.at[0],
                recv_sem=recvs.at[slot],
                device_id=partner,
                device_id_type=MESH,
            ).wait_recv()

        def forward(buffer, sends, recvs, r):
            other = ring(r)
            received(buffer, sends, recvs, nx + other)
            base = nx + 1 + 2 * (r - 1)
            sent.append(send(buffer, sends, recvs, base, nx + other, 2 * nx * c + other, partner))
            sent.append(
                send(buffer, sends, recvs, base + 1, nx + other, 2 * nx * (1 - c) + other, across)
            )

        pole_set = (poles_v, pole_send, pole_recv)
        panel_set = (panels_v, panel_send, panel_recv)
        first_sends(*pole_set)
        first_sends(*panel_set)

        loads[1].wait()

        def set_apart(part, buffer, count):
            scratch = m2l_f.at[buffer]
            unfold(m2l_v, scratch, part, count)
            for k in range(count):
                pair_v[part * group + k] = unfolded(scratch, k)

        def set_apart_all(step, carry):
            for buffer in range(buffers):
                set_apart(buffers * step + buffer, buffer, group)
            return carry

        whole = offsets // group
        steps = whole // buffers
        lax.fori_loop(0, steps // 2, set_apart_all, 0)
        forward(*pole_set, 1)
        forward(*pole_set, nx - 1)
        lax.fori_loop(steps // 2, steps, set_apart_all, 0)
        for part in range(steps * buffers, whole):
            set_apart(part, part % buffers, group)
        if offsets % group:
            set_apart(whole, whole % buffers, offsets % group)
        forward(*pole_set, nx // 2)
        forward(*panel_set, 1)
        forward(*panel_set, nx - 1)
        forward(*panel_set, nx // 2)

        valid_before = (seg > 0).astype(f32)
        valid_after = (seg < segments - 1).astype(f32)

        def outside_slots(recv):
            for k in range(nx):
                recv(k)
                recv(2 * nx + k)

        outside_slots(lambda slot: received(*pole_set, slot))

        pole_parts = []
        for slot in range(3 * nx):
            value = poles_v[slot]
            if slot < nx:
                value = value * valid_before
            if slot >= 2 * nx:
                value = value * valid_after
            pole_parts.append(value)
        pole_parts.append(jnp.zeros((wide - window, lanes), f32))
        all_poles = jnp.concatenate(pole_parts, axis=0)
        pole_high, pole_low = high_low(all_poles)
        both_poles = jnp.concatenate([pole_high, pole_low], axis=1).astype(bf16)

        def to_sums(t, carry):
            both = jnp.dot(count_v[t], both_poles, preferred_element_type=f32)
            sum_v[pl.ds(t * off_step, off_pad), :] = both[:, :lanes] + both[:, lanes:]
            return carry

        lax.fori_loop(0, leaves, to_sums, 0, unroll=6)

        def to_local(pair, running):
            lefts, rights = [], []
            for o in range(2):
                sums = sum_v[pl.ds(2 * pair + o, leaves, stride=off_step), :]
                high, low = high_low(sums)
                lefts.append(jnp.concatenate([high, low], axis=0).astype(bf16))
                rights.append(pair_v[2 * pair + o])
            return running + lax.dot_general(
                jnp.concatenate(lefts, axis=1),
                jnp.concatenate(rights, axis=1),
                NT,
                preferred_element_type=f32,
            )

        both = lax.fori_loop(
            0, offsets // 2, to_local, jnp.zeros((2 * leaves, lanes), f32), unroll=40
        )
        inside = lax.broadcasted_iota(jnp.int32, (leaves, lanes), 1) < terms
        local = tall(jnp.where(inside, both[:leaves] + both[leaves:], 0.0))
        loads[2].wait()
        plain = (((1,), (0,)), ((), ()))
        distant = per_leaf(local, l2p_v, l2p_f, plain, blank)[:leaves]

        outside_slots(lambda slot: received(*panel_set, slot))

        for slot in range(3 * nx):
            parts = [two_parts(panels_v[slot, comp] - 2.0) for comp in range(3)]
            area = panels_v[slot, 3]
            weight = area * panels_v[slot, 4] * (1.0 / four_pi)
            if slot < nx:
                weight = weight * valid_before
            if slot >= 2 * nx:
                weight = weight * valid_after
            square = sum((value[0] + value[1]) * (value[0] + value[1]) for value in parts)
            first, rest = high_low(square + area)
            second, third = high_low(rest)
            lines = [value[0] for value in parts] + [first, second, third]
            lines = list(enumerate(lines)) + [(7, weight)]
            lines += [(8 + k, value[1]) for k, value in enumerate(parts)]
            flat = right_v.reshape(window * row_step, panels)
            for k, line in lines:
                flat[pl.ds(slot * leaves * row_step + k, leaves, stride=row_step), :] = line

        near_v[...] = jnp.zeros(near_v.shape, f32)
        pair_lane = lax.broadcasted_iota(jnp.int32, (panels, lanes), 1)

        def to_near(t, carry):
            left = left_v[t]
            running = jnp.zeros((panels, panels), f32)
            for start in range(0, near, 2):
                entries = [near_ref[t, n] for n in range(start, min(start + 2, near))]
                blocks = []
                for w in entries:
                    block = right_v[w, :rows, :].astype(bf16)
                    fill = jnp.zeros((lanes - 2 * rows, panels), bf16)
                    blocks.append(jnp.concatenate([block, block, fill], axis=0))
                right = jnp.concatenate(blocks, axis=1) if len(blocks) > 1 else blocks[0]
                square = jnp.dot(left, right, preferred_element_type=f32)
                for k, w in enumerate(entries):
                    inverse = lax.rsqrt(square[:, k * panels : (k + 1) * panels])
                    running = running + inverse * right_v[w, 7:8, :]
            total = jnp.sum(running, axis=1, keepdims=True)
            near_v[...] = jnp.where(pair_lane == t, total, near_v[...])
            return carry

        lax.fori_loop(0, leaves, to_near, 0, unroll=8)
        nearby = near_v[...].T[:leaves]

        image = (0.5 * current + nearby + distant) * mask
        tile = jnp.where(tile_lane == krylov, inner_products(image), tile)
        tile = jnp.where(tile_lane == krylov + 1, full_sum(folded(image * image)), tile)

        def exchange(stage, sends, recvs, me, others, value):
            stage[me] = value
            copies = []
            for k, (slot, peer) in enumerate(others):
                copy = pltpu.make_async_remote_copy(
                    src_ref=stage.at[me],
                    dst_ref=stage.at[me],
                    send_sem=sends.at[k],
                    recv_sem=recvs.at[me],
                    device_id=peer,
                    device_id_type=MESH,
                )
                copy.start()
                copies.append(copy)
            for slot, peer in others:
                pltpu.make_async_remote_copy(
                    src_ref=stage.at[slot],
                    dst_ref=stage.at[slot],
                    send_sem=sends.at[0],
                    recv_sem=recvs.at[slot],
                    device_id=peer,
                    device_id_type=MESH,
                ).wait_recv()
            total = stage[0]
            for k in range(1, stage.shape[0]):
                total = total + stage[k]
            sent.extend(copies)
            return total

        others_a = [(ring(r) * nc + c, (y, z, c, ring(r))) for r in range(1, nx)]
        others_a += [(ring(r) * nc + 1 - c, (y, z, 1 - c, ring(r))) for r in range(nx)]
        tile = exchange(stage_a, a_send, a_recv, x * nc + c, others_a, tile)
        others_b = [(lax.rem(q + r, group_b), peers_b[r - 1]) for r in range(1, group_b)]
        tile = exchange(stage_b, b_send, b_recv, q, others_b, tile)

        def column(index):
            return jnp.sum(jnp.where(tile_lane == index, tile, 0.0), axis=1, keepdims=True)

        population = column(krylov + 2)[:1]
        products = column(krylov)
        energy = column(krylov + 1)[:1]
        coefficients = products / population
        tile_row = lax.broadcasted_iota(jnp.int32, (krylov, lanes), 0)
        spread = jnp.sum(
            jnp.where(tile_lane == tile_row, coefficients, 0.0), axis=0, keepdims=True
        )
        gram = jnp.where(tile_lane < krylov, tile, 0.0)
        curvature = full_sum(gram * coefficients * spread)
        squares = energy - 2.0 * full_sum(coefficients * products) + curvature
        scale = jnp.sqrt(squares / population + epsilon)
        residue = image
        for j in range(krylov):
            residue = residue - coefficients[j : j + 1] * masked[j]
        vec_ref[...] = residue / scale
        lane_row = lax.broadcasted_iota(jnp.int32, (1, lanes), 1)
        hess_ref[...] = jnp.where(lane_row == krylov, scale, spread)

        for copy in sent:
            copy.wait_send()

    vmem = pl.BlockSpec(memory_space=pltpu.VMEM)
    smem = pl.BlockSpec(memory_space=pltpu.SMEM)
    anywhere = pl.BlockSpec(memory_space=pl.ANY)
    dma = pltpu.SemaphoreType.DMA
    slots = 3 * nx
    n_sends = nx + 1 + 2 * (nx - 1)
    return pl.pallas_call(
        kernel,
        out_shape=(
            jax.ShapeDtypeStruct((leaves, panels), f32),
            jax.ShapeDtypeStruct((1, lanes), f32),
        ),
        in_specs=[vmem, vmem, vmem, smem, smem, vmem, vmem, anywhere, anywhere, anywhere],
        out_specs=(vmem, vmem),
        scratch_shapes=[
            pltpu.VMEM((terms, leaves, panels), bf16),
            pltpu.VMEM((terms, leaves, panels), bf16),
            pltpu.VMEM((terms, offsets, terms), bf16),
            pltpu.VMEM((slots, 5, leaves, panels), f32),
            pltpu.VMEM((slots, leaves, lanes), f32),
            pltpu.VMEM((leaves, far_pad), jnp.int32),
            pltpu.VMEM((leaves, far_pad), jnp.int32),
            pltpu.VMEM((leaves, off_pad, wide), bf16),
            pltpu.VMEM((leaves * off_step, lanes), f32),
            pltpu.VMEM((leaves, panels, lanes), bf16),
            pltpu.VMEM((window, row_step, panels), f32),
            pltpu.VMEM((leaves * part_step, panels), f32),
            pltpu.VMEM((panels, lanes), f32),
            pltpu.VMEM((folded_rows, lanes), f32),
            pltpu.VMEM((folded_rows, lanes), f32),
            pltpu.VMEM((buffers, folded_rows, lanes), f32),
            pltpu.VMEM((offsets, lanes, lanes), bf16),
            pltpu.VMEM((group_a, krylov, lanes), f32),
            pltpu.VMEM((group_b, krylov, lanes), f32),
            dma((3,)),
            dma((n_sends,)),
            dma((slots,)),
            dma((n_sends,)),
            dma((slots,)),
            dma((group_a,)),
            dma((group_a,)),
            dma((group_b,)),
            dma((group_b,)),
        ],
        compiler_params=pltpu.CompilerParams(
            collective_id=0, has_side_effects=True, vmem_limit_bytes=56 * 1024 * 1024
        ),
    )


def solution(mesh):
    torus = Mesh(mesh.devices.reshape(4, 4, 2, mesh.shape["grp"]), AXES)
    every = AXES

    def on_device(basis, coords, areas, p2m, l2p, m2l, counts, near_list, far_list, far_offset):
        krylov, leaves, panels = basis.shape
        step = make_step(
            torus.devices.shape, krylov, leaves, panels, p2m.shape[1], m2l.shape[0],
            near_list.shape[1], far_list.shape[1],
        )
        vector, hessenberg = step(
            basis, coords.transpose(1, 0, 2), areas, counts, near_list, far_list, far_offset,
            p2m.transpose(1, 0, 2), l2p.transpose(2, 0, 1), m2l.transpose(1, 0, 2),
        )
        return vector, hessenberg[0, : krylov + 1]

    in_specs = (
        P(None, every, None),
        P(every, None, None),
        P(every, None),
        P(every, None, None),
        P(every, None, None),
        P(),
        P(every),
        P(every, None),
        P(every, None),
        P(every, None),
    )
    out_specs = (P(every, None), P())
    return jax.shard_map(
        on_device, mesh=torus, in_specs=in_specs, out_specs=out_specs, check_vma=False
    )
```

```python
import math

import jax
import jax.numpy as jnp
from jax import lax
from jax.experimental import pallas as pl
from jax.experimental.pallas import tpu as pltpu
from jax.sharding import Mesh
from jax.sharding import PartitionSpec as P

Y, Z, C, X = "seg_0", "seg_1", "seg_2", "grp"
AXES = (Y, Z, C, X)
MESH = pl.DeviceIdType.MESH
NT = (((1,), (1,)), ((), ()))
four_pi = 12.566370614359172
epsilon = 1e-06
f32 = jnp.float32
bf16 = jnp.bfloat16


def round_up(value, step):
    return -(-value // step) * step


def high_low(value):
    high = value.astype(bf16).astype(f32)
    return high, value - high


def two_parts(value):
    high, low = high_low(value)
    return high, low.astype(bf16).astype(f32)


def make_step(sizes, krylov, leaves, panels, terms, offsets, near, far):
    ny, nz, nc, nx = sizes
    segments = ny * nz * nc
    window = 3 * nx * leaves
    wide = round_up(window, 128)
    off_pad = round_up(offsets, 16)
    off_step = off_pad + 4
    far_pad = round_up(far, 128)
    lanes = 128
    group_a = nx * nc
    group_b = ny * nz
    rows = 16
    row_step = 24
    part_step = 40
    group = 8
    leaf_step = group + 1
    folded_rows = round_up((lanes - 1) * leaf_step + group, 8)
    buffers = 4

    def kernel(
        basis_ref, coords_ref, areas_ref, counts_ref, near_ref, far_ref, off_ref,
        p2m_hbm, l2p_hbm, m2l_hbm,
        vec_ref, hess_ref,
        p2m_v, l2p_v, m2l_v, panels_v, poles_v, far_v, off_v, count_v, sum_v, left_v,
        right_v, part_v, near_v, p2m_f, l2p_f, m2l_f, pair_v, stage_a, stage_b,
        load_sem, pole_send, pole_recv, panel_send, panel_recv, a_send, a_recv, b_send, b_recv,
    ):
        y, z, c, x = (lax.axis_index(name) for name in AXES)
        ys = [y] + [lax.rem(y + k, ny) for k in range(1, ny)]
        zs = [z] + [lax.rem(z + k, nz) for k in range(1, nz)]
        xs = [x] + [lax.rem(x + k, nx) for k in range(1, nx)]
        q = y * nz + z
        seg = q * nc + c
        q_across = lax.rem(q + group_b - 1 + 2 * c, group_b)
        y_across, z_across = q_across // nz, lax.rem(q_across, nz)

        loads = [
            pltpu.make_async_copy(src, dst, load_sem.at[k])
            for k, (src, dst) in enumerate(((p2m_hbm, p2m_v), (m2l_hbm, m2l_v), (l2p_hbm, l2p_v)))
        ]
        for load in loads:
            load.start()

        partner = (y, z, 1 - c, x)
        across = (y_across, z_across, 1 - c, x)
        row_own = [(y, z, c, other) for other in xs]
        row_partner = [(y, z, 1 - c, other) for other in xs]
        row_across = [(y_across, z_across, 1 - c, other) for other in xs]
        peers_b = [(other_y, other_z, c, x) for other_y in ys for other_z in zs][1:]
        slots_b = [other_y * nz + other_z for other_y in ys for other_z in zs][1:]

        barrier = pltpu.get_barrier_semaphore()
        everyone = row_own[1:] + row_partner + row_across + peers_b
        for peer in everyone:
            pl.semaphore_signal(barrier, inc=1, device_id=peer, device_id_type=MESH)

        slot_rows = lax.broadcasted_iota(jnp.int32, (leaves, panels), 0)
        mask = (slot_rows < counts_ref[0]).astype(f32)
        current = basis_ref[krylov - 1] * mask
        own = nx + x
        for comp in range(3):
            panels_v[own, comp] = coords_ref[comp]
        panels_v[own, 3] = areas_ref[...]
        panels_v[own, 4] = current

        padded = round_up(leaves, 16)

        def tall(value):
            extra = jnp.zeros((padded - leaves, value.shape[1]), f32)
            return jnp.concatenate([value, extra], axis=0).astype(bf16)

        rounded = tall(current)
        loads[0].wait()

        def unfold(source, scratch, part, count):
            start = part * group
            if not isinstance(part, int):
                start = pl.multiple_of(start, group)
            block = source[:, pl.ds(start, count), :].astype(f32)
            width = block.shape[2]
            for k in range(block.shape[0]):
                scratch[k * leaf_step : k * leaf_step + count, :width] = block[k]

        def unfolded(scratch, k):
            return scratch[pl.ds(k, lanes, stride=leaf_step), :].astype(bf16)

        def per_leaf(values, source, scratch, dims, running):
            def one_group(part, running):
                unfold(source, scratch, part, group)
                for k in range(group):
                    product = lax.dot_general(
                        values, unfolded(scratch, k), dims, preferred_element_type=f32
                    )
                    row = lax.broadcasted_iota(jnp.int32, product.shape, 0)
                    running = jnp.where(row == part * group + k, product, running)
                return running

            return lax.fori_loop(0, leaves // group, one_group, running)

        blank = jnp.zeros((padded, lanes), f32)
        multipoles = per_leaf(rounded, p2m_v, p2m_f, NT, blank)
        poles_v[own] = jnp.zeros((leaves, lanes), f32)
        poles_v[own, :, :terms] = multipoles[:leaves, :terms]

        pattern = (lax.broadcasted_iota(jnp.int32, (window, rows, panels), 1) == 6).astype(f32)
        right_v[:, :rows, :] = pattern
        for scratch in (l2p_f, m2l_f):
            scratch[...] = jnp.zeros(scratch.shape, f32)

        far_v[...] = jnp.full(far_v.shape, -1, jnp.int32)
        off_v[...] = jnp.full(off_v.shape, -1, jnp.int32)
        far_v[:, :far] = far_ref[...]
        off_v[:, :far] = off_ref[...]

        def to_counts(t, carry):
            off_row = jnp.broadcast_to(off_v[pl.ds(t, 1), :], (off_pad, far_pad))
            far_row = jnp.broadcast_to(far_v[pl.ds(t, 1), :], (wide, far_pad))
            off_hot = lax.broadcasted_iota(jnp.int32, (off_pad, far_pad), 0) == off_row
            far_hot = lax.broadcasted_iota(jnp.int32, (wide, far_pad), 0) == far_row
            pairs = lax.dot_general(
                jnp.where(off_hot, 1.0, 0.0).astype(bf16),
                jnp.where(far_hot, 1.0, 0.0).astype(bf16),
                NT,
                preferred_element_type=f32,
            )
            count_v[t] = pairs.astype(bf16)
            return carry

        lax.fori_loop(0, leaves, to_counts, 0, unroll=4)

        left_v[...] = jnp.zeros(left_v.shape, bf16)
        own_comps = [panels_v[own, comp] - 2.0 for comp in range(3)]
        splits = [two_parts(value) for value in own_comps]
        norm = sum((value[0] + value[1]) * (value[0] + value[1]) for value in splits)
        norm_high, norm_low = high_low(norm)
        one = jnp.ones((leaves, panels), f32)
        zero = jnp.zeros((leaves, panels), f32)
        highs = [-2.0 * value[0] for value in splits]
        lows = [-2.0 * value[1] for value in splits]
        columns = highs + [one, one, one, norm_high, zero]
        columns += highs + [zero] * 5
        columns += lows + [zero, zero, zero, norm_low, zero]
        columns += lows + [zero] * 5
        for k, column in enumerate(columns):
            part_v[pl.ds(k, leaves, stride=part_step), :] = column

        def to_left(t, carry):
            block = part_v[pl.ds(pl.multiple_of(t * part_step, 8), 2 * rows), :]
            left_v[t, :, : 2 * rows] = block.T.astype(bf16)
            return carry

        lax.fori_loop(0, leaves, to_left, 0, unroll=4)
        tile_lane = lax.broadcasted_iota(jnp.int32, (krylov, lanes), 1)
        masked = [basis_ref[j] * mask for j in range(krylov)]

        def folded(value):
            return sum(value[8 * k : 8 * k + 8] for k in range(leaves // 8))

        def full_sum(value):
            return jnp.sum(jnp.sum(value, axis=0, keepdims=True), axis=1, keepdims=True)

        def inner_products(vector):
            lines = [
                jnp.sum(folded(masked[i] * vector), axis=0, keepdims=True) for i in range(krylov)
            ]
            return jnp.sum(jnp.concatenate(lines, axis=0), axis=1, keepdims=True)

        tile = jnp.zeros((krylov, lanes), f32)
        for j in range(krylov):
            tile = jnp.where(tile_lane == j, inner_products(masked[j]), tile)
        tile = jnp.where(tile_lane == krylov + 2, full_sum(folded(mask)), tile)

        loads[1].wait()

        def set_apart(part, buffer, count):
            scratch = m2l_f.at[buffer]
            unfold(m2l_v, scratch, part, count)
            for k in range(count):
                pair_v[part * group + k] = unfolded(scratch, k)

        def set_apart_all(step, carry):
            for buffer in range(buffers):
                set_apart(buffers * step + buffer, buffer, group)
            return carry

        whole = offsets // group
        steps = whole // buffers
        lax.fori_loop(0, steps, set_apart_all, 0)
        for part in range(steps * buffers, whole):
            set_apart(part, part % buffers, group)
        if offsets % group:
            set_apart(whole, whole % buffers, offsets % group)
        pl.semaphore_wait(barrier, len(everyone))

        def send(buffer, sends, recvs, number, source, target_slot, peer):
            copy = pltpu.make_async_remote_copy(
                src_ref=buffer.at[source],
                dst_ref=buffer.at[target_slot],
                send_sem=sends.at[number],
                recv_sem=recvs.at[target_slot],
                device_id=peer,
                device_id_type=MESH,
            )
            copy.start()
            return copy

        sent = []

        slot_partner = 2 * nx * c
        slot_across = 2 * nx * (1 - c)

        def pole_sends():
            for k in range(nx):
                buffers = (poles_v, pole_send, pole_recv)
                if k:
                    sent.append(send(*buffers, k - 1, own, own, row_own[k]))
                sent.append(send(*buffers, nx - 1 + k, own, slot_partner + x, row_partner[k]))
                sent.append(send(*buffers, 2 * nx - 1 + k, own, slot_across + x, row_across[k]))

        def panel_sends():
            buffers = (panels_v, panel_send, panel_recv)
            for k in range(1, nx):
                sent.append(send(*buffers, k - 1, own, own, row_own[k]))
            sent.append(send(*buffers, nx - 1, own, slot_partner + x, partner))
            sent.append(send(*buffers, nx, own, slot_across + x, across))

        def received(buffer, sends, recvs, slot):
            pltpu.make_async_remote_copy(
                src_ref=buffer.at[slot],
                dst_ref=buffer.at[slot],
                send_sem=sends.at[0],
                recv_sem=recvs.at[slot],
                device_id=partner,
                device_id_type=MESH,
            ).wait_recv()

        def forward(r):
            buffers = (panels_v, panel_send, panel_recv)
            received(*buffers, nx + xs[r])
            base = nx + 1 + 2 * (r - 1)
            sent.append(send(*buffers, base, nx + xs[r], slot_partner + xs[r], partner))
            sent.append(send(*buffers, base + 1, nx + xs[r], slot_across + xs[r], across))

        pole_set = (poles_v, pole_send, pole_recv)
        panel_set = (panels_v, panel_send, panel_recv)
        pole_sends()
        panel_sends()

        valid_before = (seg > 0).astype(f32)
        valid_after = (seg < segments - 1).astype(f32)

        def outside_slots(recv):
            for k in range(nx):
                recv(k)
                recv(2 * nx + k)

        for r in range(1, nx):
            received(*pole_set, nx + xs[r])
        outside_slots(lambda slot: received(*pole_set, slot))

        pole_parts = []
        for slot in range(3 * nx):
            value = poles_v[slot]
            if slot < nx:
                value = value * valid_before
            if slot >= 2 * nx:
                value = value * valid_after
            pole_parts.append(value)
        pole_parts.append(jnp.zeros((wide - window, lanes), f32))
        all_poles = jnp.concatenate(pole_parts, axis=0)
        pole_high, pole_low = high_low(all_poles)
        both_poles = jnp.concatenate([pole_high, pole_low], axis=1).astype(bf16)

        def to_sums(t, carry):
            both = jnp.dot(count_v[t], both_poles, preferred_element_type=f32)
            sum_v[pl.ds(t * off_step, off_pad), :] = both[:, :lanes] + both[:, lanes:]
            return carry

        lax.fori_loop(0, leaves // 2, to_sums, 0, unroll=6)
        forward(1)
        forward(nx - 1)
        lax.fori_loop(leaves // 2, leaves, to_sums, 0, unroll=6)
        forward(nx // 2)

        def to_local(first, count):
            lefts, rights = [], []
            for o in range(first, first + count):
                high, low = high_low(sum_v[pl.ds(o, leaves, stride=off_step), :])
                lefts.append(jnp.concatenate([high, low], axis=0).astype(bf16))
                rights.append(pair_v[o])
            return lax.dot_general(
                jnp.concatenate(lefts, axis=1),
                jnp.concatenate(rights, axis=1),
                NT,
                preferred_element_type=f32,
            )

        half = round_up(offsets // 2, 2)
        both = to_local(0, half) + to_local(half, offsets - half)
        inside = lax.broadcasted_iota(jnp.int32, (leaves, lanes), 1) < terms
        local = tall(jnp.where(inside, both[:leaves] + both[leaves:], 0.0))
        loads[2].wait()
        plain = (((1,), (0,)), ((), ()))
        distant = per_leaf(local, l2p_v, l2p_f, plain, blank)[:leaves]

        outside_slots(lambda slot: received(*panel_set, slot))

        for slot in range(3 * nx):
            parts = [two_parts(panels_v[slot, comp] - 2.0) for comp in range(3)]
            area = panels_v[slot, 3]
            weight = area * panels_v[slot, 4] * (1.0 / four_pi)
            if slot < nx:
                weight = weight * valid_before
            if slot >= 2 * nx:
                weight = weight * valid_after
            square = sum((value[0] + value[1]) * (value[0] + value[1]) for value in parts)
            first, rest = high_low(square + area)
            second, third = high_low(rest)
            lines = [value[0] for value in parts] + [first, second, third]
            lines = list(enumerate(lines)) + [(7, weight)]
            lines += [(8 + k, value[1]) for k, value in enumerate(parts)]
            flat = right_v.reshape(window * row_step, panels)
            for k, line in lines:
                flat[pl.ds(slot * leaves * row_step + k, leaves, stride=row_step), :] = line

        near_v[...] = jnp.zeros(near_v.shape, f32)
        pair_lane = lax.broadcasted_iota(jnp.int32, (panels, lanes), 1)

        def to_near(t, carry):
            left = left_v[t]
            running = jnp.zeros((panels, panels), f32)
            for start in range(0, near, 2):
                entries = [near_ref[t, n] for n in range(start, min(start + 2, near))]
                blocks = []
                for w in entries:
                    block = right_v[w, :rows, :].astype(bf16)
                    fill = jnp.zeros((lanes - 2 * rows, panels), bf16)
                    blocks.append(jnp.concatenate([block, block, fill], axis=0))
                right = jnp.concatenate(blocks, axis=1) if len(blocks) > 1 else blocks[0]
                square = jnp.dot(left, right, preferred_element_type=f32)
                for k, w in enumerate(entries):
                    inverse = lax.rsqrt(square[:, k * panels : (k + 1) * panels])
                    running = running + inverse * right_v[w, 7:8, :]
            total = jnp.sum(running, axis=1, keepdims=True)
            near_v[...] = jnp.where(pair_lane == t, total, near_v[...])
            return carry

        lax.fori_loop(0, leaves, to_near, 0, unroll=8)
        nearby = near_v[...].T[:leaves]

        image = (0.5 * current + nearby + distant) * mask
        tile = jnp.where(tile_lane == krylov, inner_products(image), tile)
        tile = jnp.where(tile_lane == krylov + 1, full_sum(folded(image * image)), tile)

        def exchange(stage, sends, recvs, me, others, value):
            stage[me] = value
            copies = []
            for k, (slot, peer) in enumerate(others):
                copy = pltpu.make_async_remote_copy(
                    src_ref=stage.at[me],
                    dst_ref=stage.at[me],
                    send_sem=sends.at[k],
                    recv_sem=recvs.at[me],
                    device_id=peer,
                    device_id_type=MESH,
                )
                copy.start()
                copies.append(copy)
            for slot, peer in others:
                pltpu.make_async_remote_copy(
                    src_ref=stage.at[slot],
                    dst_ref=stage.at[slot],
                    send_sem=sends.at[0],
                    recv_sem=recvs.at[slot],
                    device_id=peer,
                    device_id_type=MESH,
                ).wait_recv()
            total = stage[0]
            for k in range(1, stage.shape[0]):
                total = total + stage[k]
            sent.extend(copies)
            return total

        others_a = [(xs[r] * nc + c, row_own[r]) for r in range(1, nx)]
        others_a += [(xs[r] * nc + 1 - c, row_partner[r]) for r in range(nx)]
        tile = exchange(stage_a, a_send, a_recv, x * nc + c, others_a, tile)
        others_b = list(zip(slots_b, peers_b))
        tile = exchange(stage_b, b_send, b_recv, q, others_b, tile)

        def column(index):
            return jnp.sum(jnp.where(tile_lane == index, tile, 0.0), axis=1, keepdims=True)

        population = column(krylov + 2)[:1]
        products = column(krylov)
        energy = column(krylov + 1)[:1]
        coefficients = products / population
        tile_row = lax.broadcasted_iota(jnp.int32, (krylov, lanes), 0)
        spread = jnp.sum(
            jnp.where(tile_lane == tile_row, coefficients, 0.0), axis=0, keepdims=True
        )
        gram = jnp.where(tile_lane < krylov, tile, 0.0)
        curvature = full_sum(gram * coefficients * spread)
        squares = energy - 2.0 * full_sum(coefficients * products) + curvature
        scale = jnp.sqrt(squares / population + epsilon)
        residue = image
        for j in range(krylov):
            residue = residue - coefficients[j : j + 1] * masked[j]
        vec_ref[...] = residue / scale
        lane_row = lax.broadcasted_iota(jnp.int32, (1, lanes), 1)
        hess_ref[...] = jnp.where(lane_row == krylov, scale, spread)

        for copy in sent:
            copy.wait_send()

    vmem = pl.BlockSpec(memory_space=pltpu.VMEM)
    smem = pl.BlockSpec(memory_space=pltpu.SMEM)
    anywhere = pl.BlockSpec(memory_space=pl.ANY)
    dma = pltpu.SemaphoreType.DMA
    slots = 3 * nx
    n_sends = 3 * nx
    return pl.pallas_call(
        kernel,
        out_shape=(
            jax.ShapeDtypeStruct((leaves, panels), f32),
            jax.ShapeDtypeStruct((1, lanes), f32),
        ),
        in_specs=[vmem, vmem, vmem, smem, smem, vmem, vmem, anywhere, anywhere, anywhere],
        out_specs=(vmem, vmem),
        scratch_shapes=[
            pltpu.VMEM((terms, leaves, panels), bf16),
            pltpu.VMEM((terms, leaves, panels), bf16),
            pltpu.VMEM((terms, offsets, terms), bf16),
            pltpu.VMEM((slots, 5, leaves, panels), f32),
            pltpu.VMEM((slots, leaves, lanes), f32),
            pltpu.VMEM((leaves, far_pad), jnp.int32),
            pltpu.VMEM((leaves, far_pad), jnp.int32),
            pltpu.VMEM((leaves, off_pad, wide), bf16),
            pltpu.VMEM((leaves * off_step, lanes), f32),
            pltpu.VMEM((leaves, panels, lanes), bf16),
            pltpu.VMEM((window, row_step, panels), f32),
            pltpu.VMEM((leaves * part_step, panels), f32),
            pltpu.VMEM((panels, lanes), f32),
            pltpu.VMEM((folded_rows, lanes), f32),
            pltpu.VMEM((folded_rows, lanes), f32),
            pltpu.VMEM((buffers, folded_rows, lanes), f32),
            pltpu.VMEM((offsets, lanes, lanes), bf16),
            pltpu.VMEM((group_a, krylov, lanes), f32),
            pltpu.VMEM((group_b, krylov, lanes), f32),
            dma((3,)),
            dma((n_sends,)),
            dma((slots,)),
            dma((n_sends,)),
            dma((slots,)),
            dma((group_a,)),
            dma((group_a,)),
            dma((group_b,)),
            dma((group_b,)),
        ],
        compiler_params=pltpu.CompilerParams(
            collective_id=0, has_side_effects=True, vmem_limit_bytes=56 * 1024 * 1024
        ),
    )


def solution(mesh):
    torus = Mesh(mesh.devices.reshape(4, 4, 2, mesh.shape["grp"]), AXES)
    every = AXES

    def on_device(basis, coords, areas, p2m, l2p, m2l, counts, near_list, far_list, far_offset):
        krylov, leaves, panels = basis.shape
        step = make_step(
            torus.devices.shape, krylov, leaves, panels, p2m.shape[1], m2l.shape[0],
            near_list.shape[1], far_list.shape[1],
        )
        vector, hessenberg = step(
            basis, coords.transpose(1, 0, 2), areas, counts, near_list, far_list, far_offset,
            p2m.transpose(1, 0, 2), l2p.transpose(2, 0, 1), m2l.transpose(1, 0, 2),
        )
        return vector, hessenberg[0, : krylov + 1]

    in_specs = (
        P(None, every, None),
        P(every, None, None),
        P(every, None),
        P(every, None, None),
        P(every, None, None),
        P(),
        P(every),
        P(every, None),
        P(every, None),
        P(every, None),
    )
    out_specs = (P(every, None), P())
    return jax.shard_map(
        on_device, mesh=torus, in_specs=in_specs, out_specs=out_specs, check_vma=False
    )
```

```python
import math

import jax
import jax.numpy as jnp
from jax import lax
from jax.experimental import pallas as pl
from jax.experimental.pallas import tpu as pltpu
from jax.sharding import Mesh
from jax.sharding import PartitionSpec as P

Y, Z, C, X = "seg_0", "seg_1", "seg_2", "grp"
AXES = (Y, Z, C, X)
MESH = pl.DeviceIdType.MESH
NT = (((1,), (1,)), ((), ()))
four_pi = 12.566370614359172
epsilon = 1e-06
f32 = jnp.float32
bf16 = jnp.bfloat16


def round_up(value, step):
    return -(-value // step) * step


def high_low(value):
    high = value.astype(bf16).astype(f32)
    return high, value - high


def two_parts(value):
    high, low = high_low(value)
    return high, low.astype(bf16).astype(f32)


def make_step(sizes, krylov, leaves, panels, terms, offsets, near, far):
    ny, nz, nc, nx = sizes
    segments = ny * nz * nc
    window = 3 * nx * leaves
    wide = round_up(window, 128)
    off_pad = round_up(offsets, 16)
    off_step = off_pad + 4
    far_pad = round_up(far, 128)
    lanes = 128
    group_a = nx * nc
    group_b = ny * nz
    rows = 16
    row_step = 24
    part_step = 40
    group = 8
    leaf_step = group + 1
    folded_rows = round_up((lanes - 1) * leaf_step + group, 8)
    buffers = 4

    def kernel(
        basis_ref, coords_ref, areas_ref, counts_ref, near_ref, far_ref, off_ref,
        p2m_hbm, l2p_hbm, m2l_hbm,
        vec_ref, hess_ref,
        p2m_v, l2p_v, m2l_v, panels_v, poles_v, far_v, off_v, count_v, sum_v, left_v,
        right_v, part_v, near_v, p2m_f, l2p_f, m2l_f, pair_v, stage_a, stage_b,
        load_sem, pole_send, pole_recv, panel_send, panel_recv, a_send, a_recv, b_send, b_recv,
    ):
        y, z, c, x = (lax.axis_index(name) for name in AXES)
        ys = [y] + [lax.rem(y + k, ny) for k in range(1, ny)]
        zs = [z] + [lax.rem(z + k, nz) for k in range(1, nz)]
        xs = [x] + [lax.rem(x + k, nx) for k in range(1, nx)]
        q = y * nz + z
        seg = q * nc + c
        q_across = lax.rem(q + group_b - 1 + 2 * c, group_b)
        y_across, z_across = q_across // nz, lax.rem(q_across, nz)

        loads = [
            pltpu.make_async_copy(src, dst, load_sem.at[k])
            for k, (src, dst) in enumerate(((p2m_hbm, p2m_v), (m2l_hbm, m2l_v), (l2p_hbm, l2p_v)))
        ]
        for load in loads:
            load.start()

        partner = (y, z, 1 - c, x)
        across = (y_across, z_across, 1 - c, x)
        row_own = [(y, z, c, other) for other in xs]
        row_partner = [(y, z, 1 - c, other) for other in xs]
        row_across = [(y_across, z_across, 1 - c, other) for other in xs]
        peers_b = [(other_y, other_z, c, x) for other_y in ys for other_z in zs][1:]
        slots_b = [other_y * nz + other_z for other_y in ys for other_z in zs][1:]

        barrier = pltpu.get_barrier_semaphore()
        everyone = row_own[1:] + row_partner + row_across + peers_b
        for peer in everyone:
            pl.semaphore_signal(barrier, inc=1, device_id=peer, device_id_type=MESH)

        slot_rows = lax.broadcasted_iota(jnp.int32, (leaves, panels), 0)
        mask = (slot_rows < counts_ref[0]).astype(f32)
        current = basis_ref[krylov - 1] * mask
        own = nx + x
        for comp in range(3):
            panels_v[own, comp] = coords_ref[comp]
        panels_v[own, 3] = areas_ref[...]
        panels_v[own, 4] = current

        padded = round_up(leaves, 16)

        def tall(value):
            extra = jnp.zeros((padded - leaves, value.shape[1]), f32)
            return jnp.concatenate([value, extra], axis=0).astype(bf16)

        rounded = tall(current)
        loads[0].wait()

        def unfold(source, scratch, part, count):
            start = part * group
            if not isinstance(part, int):
                start = pl.multiple_of(start, group)
            block = source[:, pl.ds(start, count), :].astype(f32)
            width = block.shape[2]
            for k in range(block.shape[0]):
                scratch[k * leaf_step : k * leaf_step + count, :width] = block[k]

        def unfolded(scratch, k):
            return scratch[pl.ds(k, lanes, stride=leaf_step), :].astype(bf16)

        def per_leaf(values, source, scratch, dims, running):
            def one_group(part, running):
                unfold(source, scratch, part, group)
                for k in range(group):
                    product = lax.dot_general(
                        values, unfolded(scratch, k), dims, preferred_element_type=f32
                    )
                    row = lax.broadcasted_iota(jnp.int32, product.shape, 0)
                    running = jnp.where(row == part * group + k, product, running)
                return running

            return lax.fori_loop(0, leaves // group, one_group, running)

        blank = jnp.zeros((padded, lanes), f32)
        multipoles = per_leaf(rounded, p2m_v, p2m_f, NT, blank)
        poles_v[own] = jnp.zeros((leaves, lanes), f32)
        poles_v[own, :, :terms] = multipoles[:leaves, :terms]

        pl.semaphore_wait(barrier, len(everyone))

        def send(buffer, sends, recvs, number, source, target_slot, peer):
            copy = pltpu.make_async_remote_copy(
                src_ref=buffer.at[source],
                dst_ref=buffer.at[target_slot],
                send_sem=sends.at[number],
                recv_sem=recvs.at[target_slot],
                device_id=peer,
                device_id_type=MESH,
            )
            copy.start()
            return copy

        sent = []

        slot_partner = 2 * nx * c
        slot_across = 2 * nx * (1 - c)

        def pole_sends():
            for k in range(nx):
                buffers = (poles_v, pole_send, pole_recv)
                if k:
                    sent.append(send(*buffers, k - 1, own, own, row_own[k]))
                sent.append(send(*buffers, nx - 1 + k, own, slot_partner + x, row_partner[k]))
                sent.append(send(*buffers, 2 * nx - 1 + k, own, slot_across + x, row_across[k]))

        def panel_sends():
            buffers = (panels_v, panel_send, panel_recv)
            for k in range(1, nx):
                sent.append(send(*buffers, k - 1, own, own, row_own[k]))
            sent.append(send(*buffers, nx - 1, own, slot_partner + x, partner))
            sent.append(send(*buffers, nx, own, slot_across + x, across))

        def received(buffer, sends, recvs, slot):
            pltpu.make_async_remote_copy(
                src_ref=buffer.at[slot],
                dst_ref=buffer.at[slot],
                send_sem=sends.at[0],
                recv_sem=recvs.at[slot],
                device_id=partner,
                device_id_type=MESH,
            ).wait_recv()

        def forward(r):
            buffers = (panels_v, panel_send, panel_recv)
            received(*buffers, nx + xs[r])
            base = nx + 1 + 2 * (r - 1)
            sent.append(send(*buffers, base, nx + xs[r], slot_partner + xs[r], partner))
            sent.append(send(*buffers, base + 1, nx + xs[r], slot_across + xs[r], across))

        pole_set = (poles_v, pole_send, pole_recv)
        panel_set = (panels_v, panel_send, panel_recv)
        pole_sends()
        panel_sends()

        pattern = (lax.broadcasted_iota(jnp.int32, (window, rows, panels), 1) == 6).astype(f32)
        right_v[:, :rows, :] = pattern
        for scratch in (l2p_f, m2l_f):
            scratch[...] = jnp.zeros(scratch.shape, f32)

        far_v[...] = jnp.full(far_v.shape, -1, jnp.int32)
        off_v[...] = jnp.full(off_v.shape, -1, jnp.int32)
        far_v[:, :far] = far_ref[...]
        off_v[:, :far] = off_ref[...]

        def to_counts(t, carry):
            off_row = jnp.broadcast_to(off_v[pl.ds(t, 1), :], (off_pad, far_pad))
            far_row = jnp.broadcast_to(far_v[pl.ds(t, 1), :], (wide, far_pad))
            off_hot = lax.broadcasted_iota(jnp.int32, (off_pad, far_pad), 0) == off_row
            far_hot = lax.broadcasted_iota(jnp.int32, (wide, far_pad), 0) == far_row
            pairs = lax.dot_general(
                jnp.where(off_hot, 1.0, 0.0).astype(bf16),
                jnp.where(far_hot, 1.0, 0.0).astype(bf16),
                NT,
                preferred_element_type=f32,
            )
            count_v[t] = pairs.astype(bf16)
            return carry

        lax.fori_loop(0, leaves, to_counts, 0, unroll=4)

        left_v[...] = jnp.zeros(left_v.shape, bf16)
        own_comps = [panels_v[own, comp] - 2.0 for comp in range(3)]
        splits = [two_parts(value) for value in own_comps]
        norm = sum((value[0] + value[1]) * (value[0] + value[1]) for value in splits)
        norm_high, norm_low = high_low(norm)
        one = jnp.ones((leaves, panels), f32)
        zero = jnp.zeros((leaves, panels), f32)
        highs = [-2.0 * value[0] for value in splits]
        lows = [-2.0 * value[1] for value in splits]
        columns = highs + [one, one, one, norm_high, zero]
        columns += highs + [zero] * 5
        columns += lows + [zero, zero, zero, norm_low, zero]
        columns += lows + [zero] * 5
        for k, column in enumerate(columns):
            part_v[pl.ds(k, leaves, stride=part_step), :] = column

        def to_left(t, carry):
            block = part_v[pl.ds(pl.multiple_of(t * part_step, 8), 2 * rows), :]
            left_v[t, :, : 2 * rows] = block.T.astype(bf16)
            return carry

        lax.fori_loop(0, leaves, to_left, 0, unroll=4)
        tile_lane = lax.broadcasted_iota(jnp.int32, (krylov, lanes), 1)
        masked = [basis_ref[j] * mask for j in range(krylov)]

        def folded(value):
            return sum(value[8 * k : 8 * k + 8] for k in range(leaves // 8))

        def full_sum(value):
            return jnp.sum(jnp.sum(value, axis=0, keepdims=True), axis=1, keepdims=True)

        def inner_products(vector):
            lines = [
                jnp.sum(folded(masked[i] * vector), axis=0, keepdims=True) for i in range(krylov)
            ]
            return jnp.sum(jnp.concatenate(lines, axis=0), axis=1, keepdims=True)

        tile = jnp.zeros((krylov, lanes), f32)
        for j in range(krylov):
            tile = jnp.where(tile_lane == j, inner_products(masked[j]), tile)
        tile = jnp.where(tile_lane == krylov + 2, full_sum(folded(mask)), tile)

        forward(1)
        forward(nx - 1)
        loads[1].wait()

        def set_apart(part, buffer, count):
            scratch = m2l_f.at[buffer]
            unfold(m2l_v, scratch, part, count)
            for k in range(count):
                pair_v[part * group + k] = unfolded(scratch, k)

        def set_apart_all(step, carry):
            for buffer in range(buffers):
                set_apart(buffers * step + buffer, buffer, group)
            return carry

        whole = offsets // group
        steps = whole // buffers
        lax.fori_loop(0, steps // 2, set_apart_all, 0)
        forward(nx // 2)
        lax.fori_loop(steps // 2, steps, set_apart_all, 0)
        for part in range(steps * buffers, whole):
            set_apart(part, part % buffers, group)
        if offsets % group:
            set_apart(whole, whole % buffers, offsets % group)

        valid_before = (seg > 0).astype(f32)
        valid_after = (seg < segments - 1).astype(f32)

        def outside_slots(recv):
            for k in range(nx):
                recv(k)
                recv(2 * nx + k)

        for r in range(1, nx):
            received(*pole_set, nx + xs[r])
        outside_slots(lambda slot: received(*pole_set, slot))

        pole_parts = []
        for slot in range(3 * nx):
            value = poles_v[slot]
            if slot < nx:
                value = value * valid_before
            if slot >= 2 * nx:
                value = value * valid_after
            pole_parts.append(value)
        pole_parts.append(jnp.zeros((wide - window, lanes), f32))
        all_poles = jnp.concatenate(pole_parts, axis=0)
        pole_high, pole_low = high_low(all_poles)
        both_poles = jnp.concatenate([pole_high, pole_low], axis=1).astype(bf16)

        def to_sums(t, carry):
            both = jnp.dot(count_v[t], both_poles, preferred_element_type=f32)
            sum_v[pl.ds(t * off_step, off_pad), :] = both[:, :lanes] + both[:, lanes:]
            return carry

        lax.fori_loop(0, leaves, to_sums, 0, unroll=6)

        def to_local(first, count):
            lefts, rights = [], []
            for o in range(first, first + count):
                high, low = high_low(sum_v[pl.ds(o, leaves, stride=off_step), :])
                lefts.append(jnp.concatenate([high, low], axis=0).astype(bf16))
                rights.append(pair_v[o])
            return lax.dot_general(
                jnp.concatenate(lefts, axis=1),
                jnp.concatenate(rights, axis=1),
                NT,
                preferred_element_type=f32,
            )

        half = round_up(offsets // 2, 2)
        both = to_local(0, half) + to_local(half, offsets - half)
        inside = lax.broadcasted_iota(jnp.int32, (leaves, lanes), 1) < terms
        local = tall(jnp.where(inside, both[:leaves] + both[leaves:], 0.0))
        loads[2].wait()
        plain = (((1,), (0,)), ((), ()))
        distant = per_leaf(local, l2p_v, l2p_f, plain, blank)[:leaves]

        outside_slots(lambda slot: received(*panel_set, slot))

        for slot in range(3 * nx):
            parts = [two_parts(panels_v[slot, comp] - 2.0) for comp in range(3)]
            area = panels_v[slot, 3]
            weight = area * panels_v[slot, 4] * (1.0 / four_pi)
            if slot < nx:
                weight = weight * valid_before
            if slot >= 2 * nx:
                weight = weight * valid_after
            square = sum((value[0] + value[1]) * (value[0] + value[1]) for value in parts)
            first, rest = high_low(square + area)
            second, third = high_low(rest)
            lines = [value[0] for value in parts] + [first, second, third]
            lines = list(enumerate(lines)) + [(7, weight)]
            lines += [(8 + k, value[1]) for k, value in enumerate(parts)]
            flat = right_v.reshape(window * row_step, panels)
            for k, line in lines:
                flat[pl.ds(slot * leaves * row_step + k, leaves, stride=row_step), :] = line

        near_v[...] = jnp.zeros(near_v.shape, f32)
        pair_lane = lax.broadcasted_iota(jnp.int32, (panels, lanes), 1)

        def to_near(t, carry):
            left = left_v[t]
            running = jnp.zeros((panels, panels), f32)
            for start in range(0, near, 2):
                entries = [near_ref[t, n] for n in range(start, min(start + 2, near))]
                blocks = []
                for w in entries:
                    block = right_v[w, :rows, :].astype(bf16)
                    fill = jnp.zeros((lanes - 2 * rows, panels), bf16)
                    blocks.append(jnp.concatenate([block, block, fill], axis=0))
                right = jnp.concatenate(blocks, axis=1) if len(blocks) > 1 else blocks[0]
                square = jnp.dot(left, right, preferred_element_type=f32)
                for k, w in enumerate(entries):
                    inverse = lax.rsqrt(square[:, k * panels : (k + 1) * panels])
                    running = running + inverse * right_v[w, 7:8, :]
            total = jnp.sum(running, axis=1, keepdims=True)
            near_v[...] = jnp.where(pair_lane == t, total, near_v[...])
            return carry

        lax.fori_loop(0, leaves, to_near, 0, unroll=8)
        nearby = near_v[...].T[:leaves]

        image = (0.5 * current + nearby + distant) * mask
        tile = jnp.where(tile_lane == krylov, inner_products(image), tile)
        tile = jnp.where(tile_lane == krylov + 1, full_sum(folded(image * image)), tile)

        def exchange(stage, sends, recvs, me, others, value):
            stage[me] = value
            copies = []
            for k, (slot, peer) in enumerate(others):
                copy = pltpu.make_async_remote_copy(
                    src_ref=stage.at[me],
                    dst_ref=stage.at[me],
                    send_sem=sends.at[k],
                    recv_sem=recvs.at[me],
                    device_id=peer,
                    device_id_type=MESH,
                )
                copy.start()
                copies.append(copy)
            for slot, peer in others:
                pltpu.make_async_remote_copy(
                    src_ref=stage.at[slot],
                    dst_ref=stage.at[slot],
                    send_sem=sends.at[0],
                    recv_sem=recvs.at[slot],
                    device_id=peer,
                    device_id_type=MESH,
                ).wait_recv()
            total = stage[0]
            for k in range(1, stage.shape[0]):
                total = total + stage[k]
            sent.extend(copies)
            return total

        others_a = [(xs[r] * nc + c, row_own[r]) for r in range(1, nx)]
        others_a += [(xs[r] * nc + 1 - c, row_partner[r]) for r in range(nx)]
        tile = exchange(stage_a, a_send, a_recv, x * nc + c, others_a, tile)
        others_b = list(zip(slots_b, peers_b))
        tile = exchange(stage_b, b_send, b_recv, q, others_b, tile)

        def column(index):
            return jnp.sum(jnp.where(tile_lane == index, tile, 0.0), axis=1, keepdims=True)

        population = column(krylov + 2)[:1]
        products = column(krylov)
        energy = column(krylov + 1)[:1]
        coefficients = products / population
        tile_row = lax.broadcasted_iota(jnp.int32, (krylov, lanes), 0)
        spread = jnp.sum(
            jnp.where(tile_lane == tile_row, coefficients, 0.0), axis=0, keepdims=True
        )
        gram = jnp.where(tile_lane < krylov, tile, 0.0)
        curvature = full_sum(gram * coefficients * spread)
        squares = energy - 2.0 * full_sum(coefficients * products) + curvature
        scale = jnp.sqrt(squares / population + epsilon)
        residue = image
        for j in range(krylov):
            residue = residue - coefficients[j : j + 1] * masked[j]
        vec_ref[...] = residue / scale
        lane_row = lax.broadcasted_iota(jnp.int32, (1, lanes), 1)
        hess_ref[...] = jnp.where(lane_row == krylov, scale, spread)

        for copy in sent:
            copy.wait_send()

    vmem = pl.BlockSpec(memory_space=pltpu.VMEM)
    smem = pl.BlockSpec(memory_space=pltpu.SMEM)
    anywhere = pl.BlockSpec(memory_space=pl.ANY)
    dma = pltpu.SemaphoreType.DMA
    slots = 3 * nx
    n_sends = 3 * nx
    return pl.pallas_call(
        kernel,
        out_shape=(
            jax.ShapeDtypeStruct((leaves, panels), f32),
            jax.ShapeDtypeStruct((1, lanes), f32),
        ),
        in_specs=[vmem, vmem, vmem, smem, smem, vmem, vmem, anywhere, anywhere, anywhere],
        out_specs=(vmem, vmem),
        scratch_shapes=[
            pltpu.VMEM((terms, leaves, panels), bf16),
            pltpu.VMEM((terms, leaves, panels), bf16),
            pltpu.VMEM((terms, offsets, terms), bf16),
            pltpu.VMEM((slots, 5, leaves, panels), f32),
            pltpu.VMEM((slots, leaves, lanes), f32),
            pltpu.VMEM((leaves, far_pad), jnp.int32),
            pltpu.VMEM((leaves, far_pad), jnp.int32),
            pltpu.VMEM((leaves, off_pad, wide), bf16),
            pltpu.VMEM((leaves * off_step, lanes), f32),
            pltpu.VMEM((leaves, panels, lanes), bf16),
            pltpu.VMEM((window, row_step, panels), f32),
            pltpu.VMEM((leaves * part_step, panels), f32),
            pltpu.VMEM((panels, lanes), f32),
            pltpu.VMEM((folded_rows, lanes), f32),
            pltpu.VMEM((folded_rows, lanes), f32),
            pltpu.VMEM((buffers, folded_rows, lanes), f32),
            pltpu.VMEM((offsets, lanes, lanes), bf16),
            pltpu.VMEM((group_a, krylov, lanes), f32),
            pltpu.VMEM((group_b, krylov, lanes), f32),
            dma((3,)),
            dma((n_sends,)),
            dma((slots,)),
            dma((n_sends,)),
            dma((slots,)),
            dma((group_a,)),
            dma((group_a,)),
            dma((group_b,)),
            dma((group_b,)),
        ],
        compiler_params=pltpu.CompilerParams(
            collective_id=0, has_side_effects=True, vmem_limit_bytes=56 * 1024 * 1024
        ),
    )


def solution(mesh):
    torus = Mesh(mesh.devices.reshape(4, 4, 2, mesh.shape["grp"]), AXES)
    every = AXES

    def on_device(basis, coords, areas, p2m, l2p, m2l, counts, near_list, far_list, far_offset):
        krylov, leaves, panels = basis.shape
        step = make_step(
            torus.devices.shape, krylov, leaves, panels, p2m.shape[1], m2l.shape[0],
            near_list.shape[1], far_list.shape[1],
        )
        vector, hessenberg = step(
            basis, coords.transpose(1, 0, 2), areas, counts, near_list, far_list, far_offset,
            p2m.transpose(1, 0, 2), l2p.transpose(2, 0, 1), m2l.transpose(1, 0, 2),
        )
        return vector, hessenberg[0, : krylov + 1]

    in_specs = (
        P(None, every, None),
        P(every, None, None),
        P(every, None),
        P(every, None, None),
        P(every, None, None),
        P(),
        P(every),
        P(every, None),
        P(every, None),
        P(every, None),
    )
    out_specs = (P(every, None), P())
    return jax.shard_map(
        on_device, mesh=torus, in_specs=in_specs, out_specs=out_specs, check_vma=False
    )
```

```python
import math

import jax
import jax.numpy as jnp
from jax import lax
from jax.experimental import pallas as pl
from jax.experimental.pallas import tpu as pltpu
from jax.sharding import Mesh
from jax.sharding import PartitionSpec as P

Y, Z, C, X = "seg_0", "seg_1", "seg_2", "grp"
AXES = (Y, Z, C, X)
MESH = pl.DeviceIdType.MESH
NT = (((1,), (1,)), ((), ()))
NN = (((1,), (0,)), ((), ()))
four_pi = 12.566370614359172
epsilon = 1e-06
f32 = jnp.float32
bf16 = jnp.bfloat16


def round_up(value, step):
    return -(-value // step) * step


def high_low(value):
    high = value.astype(bf16).astype(f32)
    return high, value - high


def two_parts(value):
    high, low = high_low(value)
    return high, low.astype(bf16).astype(f32)


def make_step(sizes, krylov, leaves, panels, terms, offsets, near, far):
    ny, nz, nc, nx = sizes
    segments = ny * nz * nc
    window = 3 * nx * leaves
    wide = round_up(window, 128)
    off_pad = round_up(offsets, 16)
    off_step = off_pad + 4
    far_pad = round_up(far, 128)
    lanes = 128
    group_a = nx * nc
    group_b = ny * nz
    rows = 16
    row_step = 24
    part_step = 40
    group = 8
    leaf_step = group + 1
    folded_rows = round_up((lanes - 1) * leaf_step + group, 8)
    buffers = 4

    def kernel(
        basis_ref, coords_ref, areas_ref, counts_ref, near_ref, far_ref, off_ref,
        p2m_hbm, l2p_hbm, m2l_hbm,
        vec_ref, hess_ref,
        p2m_v, l2p_v, m2l_v, panels_v, poles_v, far_v, off_v, count_v, sum_v, left_v,
        right_v, part_v, near_v, p2m_f, l2p_f, m2l_f, pair_v, stage_a, stage_b,
        load_sem, pole_send, pole_recv, panel_send, panel_recv, a_send, a_recv, b_send, b_recv,
    ):
        y, z, c, x = (lax.axis_index(name) for name in AXES)
        ys = [y] + [lax.rem(y + k, ny) for k in range(1, ny)]
        zs = [z] + [lax.rem(z + k, nz) for k in range(1, nz)]
        xs = [x] + [lax.rem(x + k, nx) for k in range(1, nx)]
        q = y * nz + z
        seg = q * nc + c
        q_across = lax.rem(q + group_b - 1 + 2 * c, group_b)
        y_across, z_across = q_across // nz, lax.rem(q_across, nz)

        loads = [
            pltpu.make_async_copy(src, dst, load_sem.at[k])
            for k, (src, dst) in enumerate(((p2m_hbm, p2m_v), (m2l_hbm, m2l_v), (l2p_hbm, l2p_v)))
        ]
        for load in loads:
            load.start()

        partner = (y, z, 1 - c, x)
        across = (y_across, z_across, 1 - c, x)
        row_own = [(y, z, c, other) for other in xs]
        row_partner = [(y, z, 1 - c, other) for other in xs]
        row_across = [(y_across, z_across, 1 - c, other) for other in xs]
        peers_b = [(other_y, other_z, c, x) for other_y in ys for other_z in zs][1:]
        slots_b = [other_y * nz + other_z for other_y in ys for other_z in zs][1:]

        barrier = pltpu.get_barrier_semaphore()
        everyone = row_own[1:] + row_partner + row_across + peers_b
        for peer in everyone:
            pl.semaphore_signal(barrier, inc=1, device_id=peer, device_id_type=MESH)

        slot_rows = lax.broadcasted_iota(jnp.int32, (leaves, panels), 0)
        mask = (slot_rows < counts_ref[0]).astype(f32)
        current = basis_ref[krylov - 1] * mask
        own = nx + x
        for comp in range(3):
            panels_v[own, comp] = coords_ref[comp]
        panels_v[own, 3] = areas_ref[...]
        panels_v[own, 4] = current

        padded = round_up(leaves, 16)

        def tall(value):
            extra = jnp.zeros((padded - leaves, value.shape[1]), f32)
            return jnp.concatenate([value, extra], axis=0).astype(bf16)

        rounded = tall(current)
        loads[0].wait()

        def unfold(source, scratch, part, count):
            start = part * group
            if not isinstance(part, int):
                start = pl.multiple_of(start, group)
            block = source[:, pl.ds(start, count), :].astype(f32)
            width = block.shape[2]
            for k in range(block.shape[0]):
                scratch[k * leaf_step : k * leaf_step + count, :width] = block[k]

        def unfolded(scratch, k):
            return scratch[pl.ds(k, lanes, stride=leaf_step), :].astype(bf16)

        def per_leaf(values, source, scratch, dims, running):
            def one_group(part, running):
                unfold(source, scratch, part, group)
                for k in range(group):
                    product = lax.dot_general(
                        values, unfolded(scratch, k), dims, preferred_element_type=f32
                    )
                    row = lax.broadcasted_iota(jnp.int32, product.shape, 0)
                    running = jnp.where(row == part * group + k, product, running)
                return running

            return lax.fori_loop(0, leaves // group, one_group, running)

        blank = jnp.zeros((padded, lanes), f32)
        multipoles = per_leaf(rounded, p2m_v, p2m_f, NT, blank)
        poles_v[own] = jnp.zeros((leaves, lanes), f32)
        poles_v[own, :, :terms] = multipoles[:leaves, :terms]

        pl.semaphore_wait(barrier, len(everyone))

        def send(buffer, sends, recvs, number, source, target_slot, peer):
            copy = pltpu.make_async_remote_copy(
                src_ref=buffer.at[source],
                dst_ref=buffer.at[target_slot],
                send_sem=sends.at[number],
                recv_sem=recvs.at[target_slot],
                device_id=peer,
                device_id_type=MESH,
            )
            copy.start()
            return copy

        sent = []

        slot_partner = 2 * nx * c
        slot_across = 2 * nx * (1 - c)

        def pole_sends():
            for k in range(nx):
                buffers = (poles_v, pole_send, pole_recv)
                if k:
                    sent.append(send(*buffers, k - 1, own, own, row_own[k]))
                sent.append(send(*buffers, nx - 1 + k, own, slot_partner + x, row_partner[k]))
                sent.append(send(*buffers, 2 * nx - 1 + k, own, slot_across + x, row_across[k]))

        def panel_sends():
            buffers = (panels_v, panel_send, panel_recv)
            for k in range(1, nx):
                sent.append(send(*buffers, k - 1, own, own, row_own[k]))
            sent.append(send(*buffers, nx - 1, own, slot_partner + x, partner))
            sent.append(send(*buffers, nx, own, slot_across + x, across))

        def received(buffer, sends, recvs, slot):
            pltpu.make_async_remote_copy(
                src_ref=buffer.at[slot],
                dst_ref=buffer.at[slot],
                send_sem=sends.at[0],
                recv_sem=recvs.at[slot],
                device_id=partner,
                device_id_type=MESH,
            ).wait_recv()

        def forward(r):
            buffers = (panels_v, panel_send, panel_recv)
            received(*buffers, nx + xs[r])
            base = nx + 1 + 2 * (r - 1)
            sent.append(send(*buffers, base, nx + xs[r], slot_partner + xs[r], partner))
            sent.append(send(*buffers, base + 1, nx + xs[r], slot_across + xs[r], across))

        pole_set = (poles_v, pole_send, pole_recv)
        panel_set = (panels_v, panel_send, panel_recv)
        pole_sends()
        panel_sends()

        pattern = (lax.broadcasted_iota(jnp.int32, (window, rows, panels), 1) == 6).astype(f32)
        right_v[:, :rows, :] = pattern
        for scratch in (l2p_f, m2l_f):
            scratch[...] = jnp.zeros(scratch.shape, f32)

        far_v[...] = jnp.full(far_v.shape, -1, jnp.int32)
        off_v[...] = jnp.full(off_v.shape, -1, jnp.int32)
        far_v[:, :far] = far_ref[...]
        off_v[:, :far] = off_ref[...]

        def to_counts(t, carry):
            off_row = jnp.broadcast_to(off_v[pl.ds(t, 1), :], (off_pad, far_pad))
            far_row = jnp.broadcast_to(far_v[pl.ds(t, 1), :], (wide, far_pad))
            off_hot = lax.broadcasted_iota(jnp.int32, (off_pad, far_pad), 0) == off_row
            far_hot = lax.broadcasted_iota(jnp.int32, (wide, far_pad), 0) == far_row
            pairs = lax.dot_general(
                jnp.where(off_hot, 1.0, 0.0).astype(bf16),
                jnp.where(far_hot, 1.0, 0.0).astype(bf16),
                NT,
                preferred_element_type=f32,
            )
            count_v[t] = pairs.astype(bf16)
            return carry

        lax.fori_loop(0, leaves, to_counts, 0, unroll=4)

        left_v[...] = jnp.zeros(left_v.shape, bf16)
        own_comps = [panels_v[own, comp] - 2.0 for comp in range(3)]
        splits = [two_parts(value) for value in own_comps]
        norm = sum((value[0] + value[1]) * (value[0] + value[1]) for value in splits)
        norm_high, norm_low = high_low(norm)
        one = jnp.ones((leaves, panels), f32)
        zero = jnp.zeros((leaves, panels), f32)
        highs = [-2.0 * value[0] for value in splits]
        lows = [-2.0 * value[1] for value in splits]
        columns = highs + [one, one, one, norm_high, zero]
        columns += highs + [zero] * 5
        columns += lows + [zero, zero, zero, norm_low, zero]
        columns += lows + [zero] * 5
        for k, column in enumerate(columns):
            part_v[pl.ds(k, leaves, stride=part_step), :] = column

        def to_left(t, carry):
            block = part_v[pl.ds(pl.multiple_of(t * part_step, 8), 2 * rows), :]
            left_v[t, :, : 2 * rows] = block.T.astype(bf16)
            return carry

        lax.fori_loop(0, leaves, to_left, 0, unroll=4)
        tile_lane = lax.broadcasted_iota(jnp.int32, (krylov, lanes), 1)
        masked = [basis_ref[j] * mask for j in range(krylov)]

        def folded(value):
            return sum(value[8 * k : 8 * k + 8] for k in range(leaves // 8))

        def full_sum(value):
            return jnp.sum(jnp.sum(value, axis=0, keepdims=True), axis=1, keepdims=True)

        def inner_products(vector):
            lines = [
                jnp.sum(folded(masked[i] * vector), axis=0, keepdims=True) for i in range(krylov)
            ]
            return jnp.sum(jnp.concatenate(lines, axis=0), axis=1, keepdims=True)

        tile = jnp.zeros((krylov, lanes), f32)
        for j in range(krylov):
            tile = jnp.where(tile_lane == j, inner_products(masked[j]), tile)
        tile = jnp.where(tile_lane == krylov + 2, full_sum(folded(mask)), tile)

        forward(1)
        forward(nx - 1)
        loads[1].wait()

        def set_apart(part, buffer, count):
            scratch = m2l_f.at[buffer]
            unfold(m2l_v, scratch, part, count)
            for k in range(count):
                pair_v[part * group + k] = unfolded(scratch, k).T

        def set_apart_all(step, carry):
            for buffer in range(buffers):
                set_apart(buffers * step + buffer, buffer, group)
            return carry

        whole = offsets // group
        steps = whole // buffers
        lax.fori_loop(0, steps // 2, set_apart_all, 0)
        forward(nx // 2)
        lax.fori_loop(steps // 2, steps, set_apart_all, 0)
        for part in range(steps * buffers, whole):
            set_apart(part, part % buffers, group)
        if offsets % group:
            set_apart(whole, whole % buffers, offsets % group)

        valid_before = (seg > 0).astype(f32)
        valid_after = (seg < segments - 1).astype(f32)

        def outside_slots(recv):
            for k in range(nx):
                recv(k)
                recv(2 * nx + k)

        for r in range(1, nx):
            received(*pole_set, nx + xs[r])
        outside_slots(lambda slot: received(*pole_set, slot))

        pole_parts = []
        for slot in range(3 * nx):
            value = poles_v[slot]
            if slot < nx:
                value = value * valid_before
            if slot >= 2 * nx:
                value = value * valid_after
            pole_parts.append(value)
        pole_parts.append(jnp.zeros((wide - window, lanes), f32))
        all_poles = jnp.concatenate(pole_parts, axis=0)
        pole_high, pole_low = high_low(all_poles)
        both_poles = jnp.concatenate([pole_high, pole_low], axis=1).astype(bf16)

        def to_sums(t, carry):
            both = jnp.dot(count_v[t], both_poles, preferred_element_type=f32)
            sum_v[pl.ds(t * off_step, off_pad), :] = both[:, :lanes] + both[:, lanes:]
            return carry

        lax.fori_loop(0, leaves, to_sums, 0, unroll=6)

        def to_local(first, count):
            lefts, rights = [], []
            for o in range(first, first + count):
                high, low = high_low(sum_v[pl.ds(o, leaves, stride=off_step), :])
                lefts.append(jnp.concatenate([high, low], axis=0).astype(bf16))
                rights.append(pair_v[o])
            return lax.dot_general(
                jnp.concatenate(lefts, axis=1),
                jnp.concatenate(rights, axis=0),
                NN,
                preferred_element_type=f32,
            )

        half = round_up(offsets // 2, 2)
        both = to_local(0, half) + to_local(half, offsets - half)
        inside = lax.broadcasted_iota(jnp.int32, (leaves, lanes), 1) < terms
        local = tall(jnp.where(inside, both[:leaves] + both[leaves:], 0.0))
        loads[2].wait()
        distant = per_leaf(local, l2p_v, l2p_f, NN, blank)[:leaves]

        outside_slots(lambda slot: received(*panel_set, slot))

        for slot in range(3 * nx):
            parts = [two_parts(panels_v[slot, comp] - 2.0) for comp in range(3)]
            area = panels_v[slot, 3]
            weight = area * panels_v[slot, 4] * (1.0 / four_pi)
            if slot < nx:
                weight = weight * valid_before
            if slot >= 2 * nx:
                weight = weight * valid_after
            square = sum((value[0] + value[1]) * (value[0] + value[1]) for value in parts)
            first, rest = high_low(square + area)
            second, third = high_low(rest)
            lines = [value[0] for value in parts] + [first, second, third]
            lines = list(enumerate(lines)) + [(7, weight)]
            lines += [(8 + k, value[1]) for k, value in enumerate(parts)]
            flat = right_v.reshape(window * row_step, panels)
            for k, line in lines:
                flat[pl.ds(slot * leaves * row_step + k, leaves, stride=row_step), :] = line

        near_v[...] = jnp.zeros(near_v.shape, f32)
        pair_lane = lax.broadcasted_iota(jnp.int32, (panels, lanes), 1)

        def to_near(t, carry):
            left = left_v[t]
            running = jnp.zeros((panels, panels), f32)
            for start in range(0, near, 2):
                entries = [near_ref[t, n] for n in range(start, min(start + 2, near))]
                blocks = []
                for w in entries:
                    block = right_v[w, :rows, :].astype(bf16)
                    fill = jnp.zeros((lanes - 2 * rows, panels), bf16)
                    blocks.append(jnp.concatenate([block, block, fill], axis=0))
                right = jnp.concatenate(blocks, axis=1) if len(blocks) > 1 else blocks[0]
                square = jnp.dot(left, right, preferred_element_type=f32)
                for k, w in enumerate(entries):
                    inverse = lax.rsqrt(square[:, k * panels : (k + 1) * panels])
                    running = running + inverse * right_v[w, 7:8, :]
            total = jnp.sum(running, axis=1, keepdims=True)
            near_v[...] = jnp.where(pair_lane == t, total, near_v[...])
            return carry

        lax.fori_loop(0, leaves, to_near, 0, unroll=8)
        nearby = near_v[...].T[:leaves]

        image = (0.5 * current + nearby + distant) * mask
        tile = jnp.where(tile_lane == krylov, inner_products(image), tile)
        tile = jnp.where(tile_lane == krylov + 1, full_sum(folded(image * image)), tile)

        def exchange(stage, sends, recvs, me, others, value):
            stage[me] = value
            copies = []
            for k, (slot, peer) in enumerate(others):
                copy = pltpu.make_async_remote_copy(
                    src_ref=stage.at[me],
                    dst_ref=stage.at[me],
                    send_sem=sends.at[k],
                    recv_sem=recvs.at[me],
                    device_id=peer,
                    device_id_type=MESH,
                )
                copy.start()
                copies.append(copy)
            for slot, peer in others:
                pltpu.make_async_remote_copy(
                    src_ref=stage.at[slot],
                    dst_ref=stage.at[slot],
                    send_sem=sends.at[0],
                    recv_sem=recvs.at[slot],
                    device_id=peer,
                    device_id_type=MESH,
                ).wait_recv()
            total = stage[0]
            for k in range(1, stage.shape[0]):
                total = total + stage[k]
            sent.extend(copies)
            return total

        others_a = [(xs[r] * nc + c, row_own[r]) for r in range(1, nx)]
        others_a += [(xs[r] * nc + 1 - c, row_partner[r]) for r in range(nx)]
        tile = exchange(stage_a, a_send, a_recv, x * nc + c, others_a, tile)
        others_b = list(zip(slots_b, peers_b))
        tile = exchange(stage_b, b_send, b_recv, q, others_b, tile)

        def column(index):
            return jnp.sum(jnp.where(tile_lane == index, tile, 0.0), axis=1, keepdims=True)

        population = column(krylov + 2)[:1]
        products = column(krylov)
        energy = column(krylov + 1)[:1]
        coefficients = products / population
        tile_row = lax.broadcasted_iota(jnp.int32, (krylov, lanes), 0)
        spread = jnp.sum(
            jnp.where(tile_lane == tile_row, coefficients, 0.0), axis=0, keepdims=True
        )
        gram = jnp.where(tile_lane < krylov, tile, 0.0)
        curvature = full_sum(gram * coefficients * spread)
        squares = energy - 2.0 * full_sum(coefficients * products) + curvature
        scale = jnp.sqrt(squares / population + epsilon)
        residue = image
        for j in range(krylov):
            residue = residue - coefficients[j : j + 1] * masked[j]
        vec_ref[...] = residue / scale
        lane_row = lax.broadcasted_iota(jnp.int32, (1, lanes), 1)
        hess_ref[...] = jnp.where(lane_row == krylov, scale, spread)

        for copy in sent:
            copy.wait_send()

    vmem = pl.BlockSpec(memory_space=pltpu.VMEM)
    smem = pl.BlockSpec(memory_space=pltpu.SMEM)
    anywhere = pl.BlockSpec(memory_space=pl.ANY)
    dma = pltpu.SemaphoreType.DMA
    slots = 3 * nx
    n_sends = 3 * nx
    return pl.pallas_call(
        kernel,
        out_shape=(
            jax.ShapeDtypeStruct((leaves, panels), f32),
            jax.ShapeDtypeStruct((1, lanes), f32),
        ),
        in_specs=[vmem, vmem, vmem, smem, smem, vmem, vmem, anywhere, anywhere, anywhere],
        out_specs=(vmem, vmem),
        scratch_shapes=[
            pltpu.VMEM((terms, leaves, panels), bf16),
            pltpu.VMEM((terms, leaves, panels), bf16),
            pltpu.VMEM((terms, offsets, terms), bf16),
            pltpu.VMEM((slots, 5, leaves, panels), f32),
            pltpu.VMEM((slots, leaves, lanes), f32),
            pltpu.VMEM((leaves, far_pad), jnp.int32),
            pltpu.VMEM((leaves, far_pad), jnp.int32),
            pltpu.VMEM((leaves, off_pad, wide), bf16),
            pltpu.VMEM((leaves * off_step, lanes), f32),
            pltpu.VMEM((leaves, panels, lanes), bf16),
            pltpu.VMEM((window, row_step, panels), f32),
            pltpu.VMEM((leaves * part_step, panels), f32),
            pltpu.VMEM((panels, lanes), f32),
            pltpu.VMEM((folded_rows, lanes), f32),
            pltpu.VMEM((folded_rows, lanes), f32),
            pltpu.VMEM((buffers, folded_rows, lanes), f32),
            pltpu.VMEM((offsets, lanes, lanes), bf16),
            pltpu.VMEM((group_a, krylov, lanes), f32),
            pltpu.VMEM((group_b, krylov, lanes), f32),
            dma((3,)),
            dma((n_sends,)),
            dma((slots,)),
            dma((n_sends,)),
            dma((slots,)),
            dma((group_a,)),
            dma((group_a,)),
            dma((group_b,)),
            dma((group_b,)),
        ],
        compiler_params=pltpu.CompilerParams(
            collective_id=0, has_side_effects=True, vmem_limit_bytes=56 * 1024 * 1024
        ),
    )


def solution(mesh):
    torus = Mesh(mesh.devices.reshape(4, 4, 2, mesh.shape["grp"]), AXES)
    every = AXES

    def on_device(basis, coords, areas, p2m, l2p, m2l, counts, near_list, far_list, far_offset):
        krylov, leaves, panels = basis.shape
        step = make_step(
            torus.devices.shape, krylov, leaves, panels, p2m.shape[1], m2l.shape[0],
            near_list.shape[1], far_list.shape[1],
        )
        vector, hessenberg = step(
            basis, coords.transpose(1, 0, 2), areas, counts, near_list, far_list, far_offset,
            p2m.transpose(1, 0, 2), l2p.transpose(2, 0, 1), m2l.transpose(1, 0, 2),
        )
        return vector, hessenberg[0, : krylov + 1]

    in_specs = (
        P(None, every, None),
        P(every, None, None),
        P(every, None),
        P(every, None, None),
        P(every, None, None),
        P(),
        P(every),
        P(every, None),
        P(every, None),
        P(every, None),
    )
    out_specs = (P(every, None), P())
    return jax.shard_map(
        on_device, mesh=torus, in_specs=in_specs, out_specs=out_specs, check_vma=False
    )
```

```python
import math

import jax
import jax.numpy as jnp
from jax import lax
from jax.experimental import pallas as pl
from jax.experimental.pallas import tpu as pltpu
from jax.sharding import Mesh
from jax.sharding import PartitionSpec as P

Y, Z, C, X = "seg_0", "seg_1", "seg_2", "grp"
AXES = (Y, Z, C, X)
MESH = pl.DeviceIdType.MESH
NT = (((1,), (1,)), ((), ()))
NN = (((1,), (0,)), ((), ()))
four_pi = 12.566370614359172
epsilon = 1e-06
f32 = jnp.float32
bf16 = jnp.bfloat16


def round_up(value, step):
    return -(-value // step) * step


def high_low(value):
    high = value.astype(bf16).astype(f32)
    return high, value - high


def two_parts(value):
    high, low = high_low(value)
    return high, low.astype(bf16).astype(f32)


def make_step(sizes, krylov, leaves, panels, terms, offsets, near, far):
    ny, nz, nc, nx = sizes
    segments = ny * nz * nc
    window = 3 * nx * leaves
    wide = round_up(window, 128)
    off_pad = round_up(offsets, 16)
    off_step = off_pad + 4
    far_pad = round_up(far, 128)
    lanes = 128
    group_a = nx * nc
    group_b = ny * nz
    rows = 16
    row_step = 24
    part_step = 40
    group = 8
    leaf_step = group + 1
    folded_rows = round_up((lanes - 1) * leaf_step + group, 8)
    buffers = 4

    def kernel(
        basis_ref, coords_ref, areas_ref, counts_ref, near_ref, far_ref, off_ref,
        p2m_hbm, l2p_hbm, m2l_hbm,
        vec_ref, hess_ref,
        p2m_v, l2p_v, m2l_v, panels_v, poles_v, far_v, off_v, count_v, sum_v, left_v,
        right_v, part_v, near_v, p2m_f, l2p_f, m2l_f, pair_v, stage_a, stage_b,
        load_sem, pole_send, pole_recv, panel_send, panel_recv, a_send, a_recv, b_send, b_recv,
    ):
        y, z, c, x = (lax.axis_index(name) for name in AXES)
        ys = [y] + [lax.rem(y + k, ny) for k in range(1, ny)]
        zs = [z] + [lax.rem(z + k, nz) for k in range(1, nz)]
        xs = [x] + [lax.rem(x + k, nx) for k in range(1, nx)]
        q = y * nz + z
        seg = q * nc + c
        q_across = lax.rem(q + group_b - 1 + 2 * c, group_b)
        y_across, z_across = q_across // nz, lax.rem(q_across, nz)

        loads = [
            pltpu.make_async_copy(src, dst, load_sem.at[k])
            for k, (src, dst) in enumerate(((p2m_hbm, p2m_v), (m2l_hbm, m2l_v), (l2p_hbm, l2p_v)))
        ]
        for load in loads:
            load.start()

        partner = (y, z, 1 - c, x)
        across = (y_across, z_across, 1 - c, x)
        row_own = [(y, z, c, other) for other in xs]
        row_partner = [(y, z, 1 - c, other) for other in xs]
        row_across = [(y_across, z_across, 1 - c, other) for other in xs]
        peers_b = [(other_y, other_z, c, x) for other_y in ys for other_z in zs][1:]
        slots_b = [other_y * nz + other_z for other_y in ys for other_z in zs][1:]

        barrier = pltpu.get_barrier_semaphore()
        everyone = row_own[1:] + row_partner + row_across + peers_b
        for peer in everyone:
            pl.semaphore_signal(barrier, inc=1, device_id=peer, device_id_type=MESH)

        slot_rows = lax.broadcasted_iota(jnp.int32, (leaves, panels), 0)
        mask = (slot_rows < counts_ref[0]).astype(f32)
        current = basis_ref[krylov - 1] * mask
        own = nx + x
        for comp in range(3):
            panels_v[own, comp] = coords_ref[comp]
        panels_v[own, 3] = areas_ref[...]
        panels_v[own, 4] = current

        pattern = (lax.broadcasted_iota(jnp.int32, (window, rows, panels), 1) == 6).astype(f32)
        right_v[:, :rows, :] = pattern
        for scratch in (l2p_f, m2l_f):
            scratch[...] = jnp.zeros(scratch.shape, f32)


        pl.semaphore_wait(barrier, len(everyone))

        def send(buffer, sends, recvs, number, source, target_slot, peer):
            copy = pltpu.make_async_remote_copy(
                src_ref=buffer.at[source],
                dst_ref=buffer.at[target_slot],
                send_sem=sends.at[number],
                recv_sem=recvs.at[target_slot],
                device_id=peer,
                device_id_type=MESH,
            )
            copy.start()
            return copy

        sent = []

        slot_partner = 2 * nx * c
        slot_across = 2 * nx * (1 - c)

        def pole_sends():
            for k in range(nx):
                buffers = (poles_v, pole_send, pole_recv)
                if k:
                    sent.append(send(*buffers, k - 1, own, own, row_own[k]))
                sent.append(send(*buffers, nx - 1 + k, own, slot_partner + x, row_partner[k]))
                sent.append(send(*buffers, 2 * nx - 1 + k, own, slot_across + x, row_across[k]))

        def panel_sends():
            buffers = (panels_v, panel_send, panel_recv)
            for k in (nx // 2, 1, nx - 1):
                sent.append(send(*buffers, k - 1, own, own, row_own[k]))
            sent.append(send(*buffers, nx - 1, own, slot_partner + x, partner))
            sent.append(send(*buffers, nx, own, slot_across + x, across))

        def received(buffer, sends, recvs, slot):
            pltpu.make_async_remote_copy(
                src_ref=buffer.at[slot],
                dst_ref=buffer.at[slot],
                send_sem=sends.at[0],
                recv_sem=recvs.at[slot],
                device_id=partner,
                device_id_type=MESH,
            ).wait_recv()

        def forward(r):
            buffers = (panels_v, panel_send, panel_recv)
            received(*buffers, nx + xs[r])
            base = nx + 1 + 2 * (r - 1)
            sent.append(send(*buffers, base, nx + xs[r], slot_partner + xs[r], partner))
            sent.append(send(*buffers, base + 1, nx + xs[r], slot_across + xs[r], across))

        pole_set = (poles_v, pole_send, pole_recv)
        panel_set = (panels_v, panel_send, panel_recv)
        panel_sends()

        padded = round_up(leaves, 16)

        def tall(value):
            extra = jnp.zeros((padded - leaves, value.shape[1]), f32)
            return jnp.concatenate([value, extra], axis=0).astype(bf16)

        rounded = tall(current)
        loads[0].wait()

        def unfold(source, scratch, part, count):
            start = part * group
            if not isinstance(part, int):
                start = pl.multiple_of(start, group)
            block = source[:, pl.ds(start, count), :].astype(f32)
            width = block.shape[2]
            for k in range(block.shape[0]):
                scratch[k * leaf_step : k * leaf_step + count, :width] = block[k]

        def unfolded(scratch, k):
            return scratch[pl.ds(k, lanes, stride=leaf_step), :].astype(bf16)

        def per_leaf(values, source, scratch, dims, running):
            def one_group(part, running):
                unfold(source, scratch, part, group)
                for k in range(group):
                    product = lax.dot_general(
                        values, unfolded(scratch, k), dims, preferred_element_type=f32
                    )
                    row = lax.broadcasted_iota(jnp.int32, product.shape, 0)
                    running = jnp.where(row == part * group + k, product, running)
                return running

            return lax.fori_loop(0, leaves // group, one_group, running)

        blank = jnp.zeros((padded, lanes), f32)
        multipoles = per_leaf(rounded, p2m_v, p2m_f, NT, blank)
        poles_v[own] = jnp.zeros((leaves, lanes), f32)
        poles_v[own, :, :terms] = multipoles[:leaves, :terms]

        pole_sends()

        far_v[...] = jnp.full(far_v.shape, -1, jnp.int32)
        off_v[...] = jnp.full(off_v.shape, -1, jnp.int32)
        far_v[:, :far] = far_ref[...]
        off_v[:, :far] = off_ref[...]

        def to_counts(t, carry):
            off_row = jnp.broadcast_to(off_v[pl.ds(t, 1), :], (off_pad, far_pad))
            far_row = jnp.broadcast_to(far_v[pl.ds(t, 1), :], (wide, far_pad))
            off_hot = lax.broadcasted_iota(jnp.int32, (off_pad, far_pad), 0) == off_row
            far_hot = lax.broadcasted_iota(jnp.int32, (wide, far_pad), 0) == far_row
            pairs = lax.dot_general(
                jnp.where(off_hot, 1.0, 0.0).astype(bf16),
                jnp.where(far_hot, 1.0, 0.0).astype(bf16),
                NT,
                preferred_element_type=f32,
            )
            count_v[t] = pairs.astype(bf16)
            return carry

        lax.fori_loop(0, leaves, to_counts, 0, unroll=4)

        left_v[...] = jnp.zeros(left_v.shape, bf16)
        own_comps = [panels_v[own, comp] - 2.0 for comp in range(3)]
        splits = [two_parts(value) for value in own_comps]
        norm = sum((value[0] + value[1]) * (value[0] + value[1]) for value in splits)
        norm_high, norm_low = high_low(norm)
        one = jnp.ones((leaves, panels), f32)
        zero = jnp.zeros((leaves, panels), f32)
        highs = [-2.0 * value[0] for value in splits]
        lows = [-2.0 * value[1] for value in splits]
        columns = highs + [one, one, one, norm_high, zero]
        columns += highs + [zero] * 5
        columns += lows + [zero, zero, zero, norm_low, zero]
        columns += lows + [zero] * 5
        for k, column in enumerate(columns):
            part_v[pl.ds(k, leaves, stride=part_step), :] = column

        def to_left(t, carry):
            block = part_v[pl.ds(pl.multiple_of(t * part_step, 8), 2 * rows), :]
            left_v[t, :, : 2 * rows] = block.T.astype(bf16)
            return carry

        lax.fori_loop(0, leaves, to_left, 0, unroll=4)
        tile_lane = lax.broadcasted_iota(jnp.int32, (krylov, lanes), 1)
        masked = [basis_ref[j] * mask for j in range(krylov)]

        def folded(value):
            return sum(value[8 * k : 8 * k + 8] for k in range(leaves // 8))

        def full_sum(value):
            return jnp.sum(jnp.sum(value, axis=0, keepdims=True), axis=1, keepdims=True)

        def inner_products(vector):
            lines = [
                jnp.sum(folded(masked[i] * vector), axis=0, keepdims=True) for i in range(krylov)
            ]
            return jnp.sum(jnp.concatenate(lines, axis=0), axis=1, keepdims=True)

        tile = jnp.zeros((krylov, lanes), f32)
        for j in range(krylov):
            tile = jnp.where(tile_lane == j, inner_products(masked[j]), tile)
        tile = jnp.where(tile_lane == krylov + 2, full_sum(folded(mask)), tile)

        forward(1)
        loads[1].wait()

        def set_apart(part, buffer, count):
            scratch = m2l_f.at[buffer]
            unfold(m2l_v, scratch, part, count)
            for k in range(count):
                pair_v[part * group + k] = unfolded(scratch, k).T

        def set_apart_all(step, carry):
            for buffer in range(buffers):
                set_apart(buffers * step + buffer, buffer, group)
            return carry

        whole = offsets // group
        steps = whole // buffers
        lax.fori_loop(0, steps // 2, set_apart_all, 0)
        forward(nx - 1)
        forward(nx // 2)
        lax.fori_loop(steps // 2, steps, set_apart_all, 0)
        for part in range(steps * buffers, whole):
            set_apart(part, part % buffers, group)
        if offsets % group:
            set_apart(whole, whole % buffers, offsets % group)

        valid_before = (seg > 0).astype(f32)
        valid_after = (seg < segments - 1).astype(f32)

        def outside_slots(recv):
            for k in range(nx):
                recv(k)
                recv(2 * nx + k)

        for r in range(1, nx):
            received(*pole_set, nx + xs[r])
        outside_slots(lambda slot: received(*pole_set, slot))

        pole_parts = []
        for slot in range(3 * nx):
            value = poles_v[slot]
            if slot < nx:
                value = value * valid_before
            if slot >= 2 * nx:
                value = value * valid_after
            pole_parts.append(value)
        pole_parts.append(jnp.zeros((wide - window, lanes), f32))
        all_poles = jnp.concatenate(pole_parts, axis=0)
        pole_high, pole_low = high_low(all_poles)
        both_poles = jnp.concatenate([pole_high, pole_low], axis=1).astype(bf16)

        def to_sums(t, carry):
            both = jnp.dot(count_v[t], both_poles, preferred_element_type=f32)
            sum_v[pl.ds(t * off_step, off_pad), :] = both[:, :lanes] + both[:, lanes:]
            return carry

        lax.fori_loop(0, leaves, to_sums, 0, unroll=6)

        def to_local(first, count):
            lefts, rights = [], []
            for o in range(first, first + count):
                high, low = high_low(sum_v[pl.ds(o, leaves, stride=off_step), :])
                lefts.append(jnp.concatenate([high, low], axis=0).astype(bf16))
                rights.append(pair_v[o])
            return lax.dot_general(
                jnp.concatenate(lefts, axis=1),
                jnp.concatenate(rights, axis=0),
                NN,
                preferred_element_type=f32,
            )

        half = round_up(offsets // 2, 2)
        both = to_local(0, half) + to_local(half, offsets - half)
        inside = lax.broadcasted_iota(jnp.int32, (leaves, lanes), 1) < terms
        local = tall(jnp.where(inside, both[:leaves] + both[leaves:], 0.0))
        loads[2].wait()
        distant = per_leaf(local, l2p_v, l2p_f, NN, blank)[:leaves]

        outside_slots(lambda slot: received(*panel_set, slot))

        for slot in range(3 * nx):
            parts = [two_parts(panels_v[slot, comp] - 2.0) for comp in range(3)]
            area = panels_v[slot, 3]
            weight = area * panels_v[slot, 4] * (1.0 / four_pi)
            if slot < nx:
                weight = weight * valid_before
            if slot >= 2 * nx:
                weight = weight * valid_after
            square = sum((value[0] + value[1]) * (value[0] + value[1]) for value in parts)
            first, rest = high_low(square + area)
            second, third = high_low(rest)
            lines = [value[0] for value in parts] + [first, second, third]
            lines = list(enumerate(lines)) + [(7, weight)]
            lines += [(8 + k, value[1]) for k, value in enumerate(parts)]
            flat = right_v.reshape(window * row_step, panels)
            for k, line in lines:
                flat[pl.ds(slot * leaves * row_step + k, leaves, stride=row_step), :] = line

        near_v[...] = jnp.zeros(near_v.shape, f32)
        pair_lane = lax.broadcasted_iota(jnp.int32, (panels, lanes), 1)

        def to_near(t, carry):
            left = left_v[t]
            running = jnp.zeros((panels, panels), f32)
            for start in range(0, near, 2):
                entries = [near_ref[t, n] for n in range(start, min(start + 2, near))]
                blocks = []
                for w in entries:
                    block = right_v[w, :rows, :].astype(bf16)
                    fill = jnp.zeros((lanes - 2 * rows, panels), bf16)
                    blocks.append(jnp.concatenate([block, block, fill], axis=0))
                right = jnp.concatenate(blocks, axis=1) if len(blocks) > 1 else blocks[0]
                square = jnp.dot(left, right, preferred_element_type=f32)
                for k, w in enumerate(entries):
                    inverse = lax.rsqrt(square[:, k * panels : (k + 1) * panels])
                    running = running + inverse * right_v[w, 7:8, :]
            total = jnp.sum(running, axis=1, keepdims=True)
            near_v[...] = jnp.where(pair_lane == t, total, near_v[...])
            return carry

        lax.fori_loop(0, leaves, to_near, 0, unroll=8)
        nearby = near_v[...].T[:leaves]

        image = (0.5 * current + nearby + distant) * mask
        tile = jnp.where(tile_lane == krylov, inner_products(image), tile)
        tile = jnp.where(tile_lane == krylov + 1, full_sum(folded(image * image)), tile)

        def exchange(stage, sends, recvs, me, others, value):
            stage[me] = value
            copies = []
            for k, (slot, peer) in enumerate(others):
                copy = pltpu.make_async_remote_copy(
                    src_ref=stage.at[me],
                    dst_ref=stage.at[me],
                    send_sem=sends.at[k],
                    recv_sem=recvs.at[me],
                    device_id=peer,
                    device_id_type=MESH,
                )
                copy.start()
                copies.append(copy)
            for slot, peer in others:
                pltpu.make_async_remote_copy(
                    src_ref=stage.at[slot],
                    dst_ref=stage.at[slot],
                    send_sem=sends.at[0],
                    recv_sem=recvs.at[slot],
                    device_id=peer,
                    device_id_type=MESH,
                ).wait_recv()
            total = stage[0]
            for k in range(1, stage.shape[0]):
                total = total + stage[k]
            sent.extend(copies)
            return total

        others_a = [(xs[r] * nc + c, row_own[r]) for r in range(1, nx)]
        others_a += [(xs[r] * nc + 1 - c, row_partner[r]) for r in range(nx)]
        tile = exchange(stage_a, a_send, a_recv, x * nc + c, others_a, tile)
        others_b = list(zip(slots_b, peers_b))
        tile = exchange(stage_b, b_send, b_recv, q, others_b, tile)

        def column(index):
            return jnp.sum(jnp.where(tile_lane == index, tile, 0.0), axis=1, keepdims=True)

        population = column(krylov + 2)[:1]
        products = column(krylov)
        energy = column(krylov + 1)[:1]
        coefficients = products / population
        tile_row = lax.broadcasted_iota(jnp.int32, (krylov, lanes), 0)
        spread = jnp.sum(
            jnp.where(tile_lane == tile_row, coefficients, 0.0), axis=0, keepdims=True
        )
        gram = jnp.where(tile_lane < krylov, tile, 0.0)
        curvature = full_sum(gram * coefficients * spread)
        squares = energy - 2.0 * full_sum(coefficients * products) + curvature
        scale = jnp.sqrt(squares / population + epsilon)
        residue = image
        for j in range(krylov):
            residue = residue - coefficients[j : j + 1] * masked[j]
        vec_ref[...] = residue / scale
        lane_row = lax.broadcasted_iota(jnp.int32, (1, lanes), 1)
        hess_ref[...] = jnp.where(lane_row == krylov, scale, spread)

        for copy in sent:
            copy.wait_send()

    vmem = pl.BlockSpec(memory_space=pltpu.VMEM)
    smem = pl.BlockSpec(memory_space=pltpu.SMEM)
    anywhere = pl.BlockSpec(memory_space=pl.ANY)
    dma = pltpu.SemaphoreType.DMA
    slots = 3 * nx
    n_sends = 3 * nx
    return pl.pallas_call(
        kernel,
        out_shape=(
            jax.ShapeDtypeStruct((leaves, panels), f32),
            jax.ShapeDtypeStruct((1, lanes), f32),
        ),
        in_specs=[vmem, vmem, vmem, smem, smem, vmem, vmem, anywhere, anywhere, anywhere],
        out_specs=(vmem, vmem),
        scratch_shapes=[
            pltpu.VMEM((terms, leaves, panels), bf16),
            pltpu.VMEM((terms, leaves, panels), bf16),
            pltpu.VMEM((terms, offsets, terms), bf16),
            pltpu.VMEM((slots, 5, leaves, panels), f32),
            pltpu.VMEM((slots, leaves, lanes), f32),
            pltpu.VMEM((leaves, far_pad), jnp.int32),
            pltpu.VMEM((leaves, far_pad), jnp.int32),
            pltpu.VMEM((leaves, off_pad, wide), bf16),
            pltpu.VMEM((leaves * off_step, lanes), f32),
            pltpu.VMEM((leaves, panels, lanes), bf16),
            pltpu.VMEM((window, row_step, panels), f32),
            pltpu.VMEM((leaves * part_step, panels), f32),
            pltpu.VMEM((panels, lanes), f32),
            pltpu.VMEM((folded_rows, lanes), f32),
            pltpu.VMEM((folded_rows, lanes), f32),
            pltpu.VMEM((buffers, folded_rows, lanes), f32),
            pltpu.VMEM((offsets, lanes, lanes), bf16),
            pltpu.VMEM((group_a, krylov, lanes), f32),
            pltpu.VMEM((group_b, krylov, lanes), f32),
            dma((3,)),
            dma((n_sends,)),
            dma((slots,)),
            dma((n_sends,)),
            dma((slots,)),
            dma((group_a,)),
            dma((group_a,)),
            dma((group_b,)),
            dma((group_b,)),
        ],
        compiler_params=pltpu.CompilerParams(
            collective_id=0, has_side_effects=True, vmem_limit_bytes=56 * 1024 * 1024
        ),
    )


def solution(mesh):
    torus = Mesh(mesh.devices.reshape(4, 4, 2, mesh.shape["grp"]), AXES)
    every = AXES

    def on_device(basis, coords, areas, p2m, l2p, m2l, counts, near_list, far_list, far_offset):
        krylov, leaves, panels = basis.shape
        step = make_step(
            torus.devices.shape, krylov, leaves, panels, p2m.shape[1], m2l.shape[0],
            near_list.shape[1], far_list.shape[1],
        )
        vector, hessenberg = step(
            basis, coords.transpose(1, 0, 2), areas, counts, near_list, far_list, far_offset,
            p2m.transpose(1, 0, 2), l2p.transpose(2, 0, 1), m2l.transpose(1, 0, 2),
        )
        return vector, hessenberg[0, : krylov + 1]

    in_specs = (
        P(None, every, None),
        P(every, None, None),
        P(every, None),
        P(every, None, None),
        P(every, None, None),
        P(),
        P(every),
        P(every, None),
        P(every, None),
        P(every, None),
    )
    out_specs = (P(every, None), P())
    return jax.shard_map(
        on_device, mesh=torus, in_specs=in_specs, out_specs=out_specs, check_vma=False
    )
```

```python
import math

import jax
import jax.numpy as jnp
from jax import lax
from jax.experimental import pallas as pl
from jax.experimental.pallas import tpu as pltpu
from jax.sharding import Mesh
from jax.sharding import PartitionSpec as P

Y, Z, C, X = "seg_0", "seg_1", "seg_2", "grp"
AXES = (Y, Z, C, X)
MESH = pl.DeviceIdType.MESH
NT = (((1,), (1,)), ((), ()))
NN = (((1,), (0,)), ((), ()))
four_pi = 12.566370614359172
epsilon = 1e-06
f32 = jnp.float32
bf16 = jnp.bfloat16


def round_up(value, step):
    return -(-value // step) * step


def high_low(value):
    high = value.astype(bf16).astype(f32)
    return high, value - high


def two_parts(value):
    high, low = high_low(value)
    return high, low.astype(bf16).astype(f32)


def make_step(sizes, krylov, leaves, panels, terms, offsets, near, far):
    ny, nz, nc, nx = sizes
    segments = ny * nz * nc
    window = 3 * nx * leaves
    wide = round_up(window, 128)
    off_pad = round_up(offsets, 16)
    off_step = off_pad + 4
    far_pad = round_up(far, 128)
    lanes = 128
    group_a = nx * nc
    group_b = ny * nz
    rows = 16
    row_step = 24
    part_step = 40
    group = 8
    leaf_step = group + 1
    folded_rows = round_up((lanes - 1) * leaf_step + group, 8)
    buffers = 8

    def kernel(
        basis_ref, coords_ref, areas_ref, counts_ref, near_ref, far_ref, off_ref,
        p2m_hbm, l2p_hbm, m2l_hbm,
        vec_ref, hess_ref,
        p2m_v, l2p_v, m2l_v, panels_v, poles_v, far_v, off_v, count_v, sum_v, left_v,
        right_v, part_v, near_v, p2m_f, l2p_f, m2l_f, pair_v, stage_a, stage_b,
        load_sem, pole_send, pole_recv, panel_send, panel_recv, a_send, a_recv, b_send, b_recv,
    ):
        y, z, c, x = (lax.axis_index(name) for name in AXES)
        ys = [y] + [lax.rem(y + k, ny) for k in range(1, ny)]
        zs = [z] + [lax.rem(z + k, nz) for k in range(1, nz)]
        xs = [x] + [lax.rem(x + k, nx) for k in range(1, nx)]
        q = y * nz + z
        seg = q * nc + c
        q_across = lax.rem(q + group_b - 1 + 2 * c, group_b)
        y_across, z_across = q_across // nz, lax.rem(q_across, nz)

        loads = [
            pltpu.make_async_copy(src, dst, load_sem.at[k])
            for k, (src, dst) in enumerate(((p2m_hbm, p2m_v), (m2l_hbm, m2l_v), (l2p_hbm, l2p_v)))
        ]
        for load in loads:
            load.start()

        partner = (y, z, 1 - c, x)
        across = (y_across, z_across, 1 - c, x)
        row_own = [(y, z, c, other) for other in xs]
        row_partner = [(y, z, 1 - c, other) for other in xs]
        row_across = [(y_across, z_across, 1 - c, other) for other in xs]
        peers_b = [(other_y, other_z, c, x) for other_y in ys for other_z in zs][1:]
        slots_b = [other_y * nz + other_z for other_y in ys for other_z in zs][1:]

        barrier = pltpu.get_barrier_semaphore()
        everyone = row_own[1:] + row_partner + row_across + peers_b
        for peer in everyone:
            pl.semaphore_signal(barrier, inc=1, device_id=peer, device_id_type=MESH)

        slot_rows = lax.broadcasted_iota(jnp.int32, (leaves, panels), 0)
        mask = (slot_rows < counts_ref[0]).astype(f32)
        current = basis_ref[krylov - 1] * mask
        own = nx + x
        for comp in range(3):
            panels_v[own, comp] = coords_ref[comp]
        panels_v[own, 3] = areas_ref[...]
        panels_v[own, 4] = current

        pattern = (lax.broadcasted_iota(jnp.int32, (window, rows, panels), 1) == 6).astype(f32)
        right_v[:, :rows, :] = pattern
        for scratch in (l2p_f, m2l_f):
            scratch[...] = jnp.zeros(scratch.shape, f32)


        pl.semaphore_wait(barrier, len(everyone))

        def send(buffer, sends, recvs, number, source, target_slot, peer):
            copy = pltpu.make_async_remote_copy(
                src_ref=buffer.at[source],
                dst_ref=buffer.at[target_slot],
                send_sem=sends.at[number],
                recv_sem=recvs.at[target_slot],
                device_id=peer,
                device_id_type=MESH,
            )
            copy.start()
            return copy

        sent = []

        slot_partner = 2 * nx * c
        slot_across = 2 * nx * (1 - c)

        def pole_sends():
            for k in range(nx):
                buffers = (poles_v, pole_send, pole_recv)
                if k:
                    sent.append(send(*buffers, k - 1, own, own, row_own[k]))
                sent.append(send(*buffers, nx - 1 + k, own, slot_partner + x, row_partner[k]))
                sent.append(send(*buffers, 2 * nx - 1 + k, own, slot_across + x, row_across[k]))

        def panel_sends():
            buffers = (panels_v, panel_send, panel_recv)
            for k in (nx // 2, 1, nx - 1):
                sent.append(send(*buffers, k - 1, own, own, row_own[k]))
            sent.append(send(*buffers, nx - 1, own, slot_partner + x, partner))
            sent.append(send(*buffers, nx, own, slot_across + x, across))

        def received(buffer, sends, recvs, slot):
            pltpu.make_async_remote_copy(
                src_ref=buffer.at[slot],
                dst_ref=buffer.at[slot],
                send_sem=sends.at[0],
                recv_sem=recvs.at[slot],
                device_id=partner,
                device_id_type=MESH,
            ).wait_recv()

        def forward(r):
            buffers = (panels_v, panel_send, panel_recv)
            received(*buffers, nx + xs[r])
            base = nx + 1 + 2 * (r - 1)
            sent.append(send(*buffers, base, nx + xs[r], slot_partner + xs[r], partner))
            sent.append(send(*buffers, base + 1, nx + xs[r], slot_across + xs[r], across))

        pole_set = (poles_v, pole_send, pole_recv)
        panel_set = (panels_v, panel_send, panel_recv)
        panel_sends()

        padded = round_up(leaves, 16)

        def tall(value):
            extra = jnp.zeros((padded - leaves, value.shape[1]), f32)
            return jnp.concatenate([value, extra], axis=0).astype(bf16)

        rounded = tall(current)
        loads[0].wait()

        def unfold(source, scratch, part, count):
            start = part * group
            if not isinstance(part, int):
                start = pl.multiple_of(start, group)
            block = source[:, pl.ds(start, count), :].astype(f32)
            width = block.shape[2]
            for k in range(block.shape[0]):
                scratch[k * leaf_step : k * leaf_step + count, :width] = block[k]

        def unfolded(scratch, k):
            return scratch[pl.ds(k, lanes, stride=leaf_step), :].astype(bf16)

        def per_leaf(values, source, scratch, dims, running):
            for part in range(leaves // group):
                unfold(source, scratch.at[part], part, group)
            for part in range(leaves // group):
                for k in range(group):
                    product = lax.dot_general(
                        values, unfolded(scratch.at[part], k), dims, preferred_element_type=f32
                    )
                    row = lax.broadcasted_iota(jnp.int32, product.shape, 0)
                    running = jnp.where(row == part * group + k, product, running)
            return running

        blank = jnp.zeros((padded, lanes), f32)
        multipoles = per_leaf(rounded, p2m_v, p2m_f, NT, blank)
        poles_v[own] = jnp.zeros((leaves, lanes), f32)
        poles_v[own, :, :terms] = multipoles[:leaves, :terms]

        pole_sends()

        far_v[...] = jnp.full(far_v.shape, -1, jnp.int32)
        off_v[...] = jnp.full(off_v.shape, -1, jnp.int32)
        far_v[:, :far] = far_ref[...]
        off_v[:, :far] = off_ref[...]

        def to_counts(t, carry):
            off_row = jnp.broadcast_to(off_v[pl.ds(t, 1), :], (off_pad, far_pad))
            far_row = jnp.broadcast_to(far_v[pl.ds(t, 1), :], (wide, far_pad))
            off_hot = lax.broadcasted_iota(jnp.int32, (off_pad, far_pad), 0) == off_row
            far_hot = lax.broadcasted_iota(jnp.int32, (wide, far_pad), 0) == far_row
            pairs = lax.dot_general(
                jnp.where(off_hot, 1.0, 0.0).astype(bf16),
                jnp.where(far_hot, 1.0, 0.0).astype(bf16),
                NT,
                preferred_element_type=f32,
            )
            count_v[t] = pairs.astype(bf16)
            return carry

        lax.fori_loop(0, leaves, to_counts, 0, unroll=6)

        left_v[...] = jnp.zeros(left_v.shape, bf16)
        own_comps = [panels_v[own, comp] - 2.0 for comp in range(3)]
        splits = [two_parts(value) for value in own_comps]
        norm = sum((value[0] + value[1]) * (value[0] + value[1]) for value in splits)
        norm_high, norm_low = high_low(norm)
        one = jnp.ones((leaves, panels), f32)
        zero = jnp.zeros((leaves, panels), f32)
        highs = [-2.0 * value[0] for value in splits]
        lows = [-2.0 * value[1] for value in splits]
        columns = highs + [one, one, one, norm_high, zero]
        columns += highs + [zero] * 5
        columns += lows + [zero, zero, zero, norm_low, zero]
        columns += lows + [zero] * 5
        for k, column in enumerate(columns):
            part_v[pl.ds(k, leaves, stride=part_step), :] = column

        def to_left(t, carry):
            block = part_v[pl.ds(pl.multiple_of(t * part_step, 8), 2 * rows), :]
            left_v[t, :, : 2 * rows] = block.T.astype(bf16)
            return carry

        lax.fori_loop(0, leaves, to_left, 0, unroll=4)
        tile_lane = lax.broadcasted_iota(jnp.int32, (krylov, lanes), 1)
        masked = [basis_ref[j] * mask for j in range(krylov)]

        def folded(value):
            return sum(value[8 * k : 8 * k + 8] for k in range(leaves // 8))

        def full_sum(value):
            return jnp.sum(jnp.sum(value, axis=0, keepdims=True), axis=1, keepdims=True)

        def inner_products(vector):
            lines = [
                jnp.sum(folded(masked[i] * vector), axis=0, keepdims=True) for i in range(krylov)
            ]
            return jnp.sum(jnp.concatenate(lines, axis=0), axis=1, keepdims=True)

        tile = jnp.zeros((krylov, lanes), f32)
        for j in range(krylov):
            tile = jnp.where(tile_lane == j, inner_products(masked[j]), tile)
        tile = jnp.where(tile_lane == krylov + 2, full_sum(folded(mask)), tile)

        forward(1)
        loads[1].wait()

        def set_apart(part, buffer, count):
            scratch = m2l_f.at[buffer]
            unfold(m2l_v, scratch, part, count)
            for k in range(count):
                pair_v[part * group + k] = unfolded(scratch, k).T

        def set_apart_all(step, carry):
            for buffer in range(buffers):
                set_apart(buffers * step + buffer, buffer, group)
            return carry

        whole = offsets // group
        steps = whole // buffers
        lax.fori_loop(0, steps // 2, set_apart_all, 0)
        forward(nx - 1)
        forward(nx // 2)
        lax.fori_loop(steps // 2, steps, set_apart_all, 0)
        for part in range(steps * buffers, whole):
            set_apart(part, part % buffers, group)
        if offsets % group:
            set_apart(whole, whole % buffers, offsets % group)

        valid_before = (seg > 0).astype(f32)
        valid_after = (seg < segments - 1).astype(f32)

        def outside_slots(recv):
            for k in range(nx):
                recv(k)
                recv(2 * nx + k)

        for r in range(1, nx):
            received(*pole_set, nx + xs[r])
        outside_slots(lambda slot: received(*pole_set, slot))

        pole_parts = []
        for slot in range(3 * nx):
            value = poles_v[slot]
            if slot < nx:
                value = value * valid_before
            if slot >= 2 * nx:
                value = value * valid_after
            pole_parts.append(value)
        pole_parts.append(jnp.zeros((wide - window, lanes), f32))
        all_poles = jnp.concatenate(pole_parts, axis=0)
        pole_high, pole_low = high_low(all_poles)
        both_poles = jnp.concatenate([pole_high, pole_low], axis=1).astype(bf16)

        def to_sums(t, carry):
            both = jnp.dot(count_v[t], both_poles, preferred_element_type=f32)
            sum_v[pl.ds(t * off_step, off_pad), :] = both[:, :lanes] + both[:, lanes:]
            return carry

        lax.fori_loop(0, leaves, to_sums, 0, unroll=12)

        def to_local(first, count):
            lefts, rights = [], []
            for o in range(first, first + count):
                high, low = high_low(sum_v[pl.ds(o, leaves, stride=off_step), :])
                lefts.append(jnp.concatenate([high, low], axis=0).astype(bf16))
                rights.append(pair_v[o])
            return lax.dot_general(
                jnp.concatenate(lefts, axis=1),
                jnp.concatenate(rights, axis=0),
                NN,
                preferred_element_type=f32,
            )

        half = round_up(offsets // 2, 2)
        both = to_local(0, half) + to_local(half, offsets - half)
        inside = lax.broadcasted_iota(jnp.int32, (leaves, lanes), 1) < terms
        local = tall(jnp.where(inside, both[:leaves] + both[leaves:], 0.0))
        loads[2].wait()
        distant = per_leaf(local, l2p_v, l2p_f, NN, blank)[:leaves]

        outside_slots(lambda slot: received(*panel_set, slot))

        for slot in range(3 * nx):
            parts = [two_parts(panels_v[slot, comp] - 2.0) for comp in range(3)]
            area = panels_v[slot, 3]
            weight = area * panels_v[slot, 4] * (1.0 / four_pi)
            if slot < nx:
                weight = weight * valid_before
            if slot >= 2 * nx:
                weight = weight * valid_after
            square = sum((value[0] + value[1]) * (value[0] + value[1]) for value in parts)
            first, rest = high_low(square + area)
            second, third = high_low(rest)
            lines = [value[0] for value in parts] + [first, second, third]
            lines = list(enumerate(lines)) + [(7, weight)]
            lines += [(8 + k, value[1]) for k, value in enumerate(parts)]
            flat = right_v.reshape(window * row_step, panels)
            for k, line in lines:
                flat[pl.ds(slot * leaves * row_step + k, leaves, stride=row_step), :] = line

        near_v[...] = jnp.zeros(near_v.shape, f32)
        pair_lane = lax.broadcasted_iota(jnp.int32, (panels, lanes), 1)

        def to_near(t, carry):
            left = left_v[t]
            running = jnp.zeros((panels, panels), f32)
            for start in range(0, near, 2):
                entries = [near_ref[t, n] for n in range(start, min(start + 2, near))]
                blocks = []
                for w in entries:
                    block = right_v[w, :rows, :].astype(bf16)
                    fill = jnp.zeros((lanes - 2 * rows, panels), bf16)
                    blocks.append(jnp.concatenate([block, block, fill], axis=0))
                right = jnp.concatenate(blocks, axis=1) if len(blocks) > 1 else blocks[0]
                square = jnp.dot(left, right, preferred_element_type=f32)
                for k, w in enumerate(entries):
                    inverse = lax.rsqrt(square[:, k * panels : (k + 1) * panels])
                    running = running + inverse * right_v[w, 7:8, :]
            total = jnp.sum(running, axis=1, keepdims=True)
            near_v[...] = jnp.where(pair_lane == t, total, near_v[...])
            return carry

        lax.fori_loop(0, leaves, to_near, 0, unroll=12)
        nearby = near_v[...].T[:leaves]

        image = (0.5 * current + nearby + distant) * mask
        tile = jnp.where(tile_lane == krylov, inner_products(image), tile)
        tile = jnp.where(tile_lane == krylov + 1, full_sum(folded(image * image)), tile)

        def exchange(stage, sends, recvs, me, others, value):
            stage[me] = value
            copies = []
            for k, (slot, peer) in enumerate(others):
                copy = pltpu.make_async_remote_copy(
                    src_ref=stage.at[me],
                    dst_ref=stage.at[me],
                    send_sem=sends.at[k],
                    recv_sem=recvs.at[me],
                    device_id=peer,
                    device_id_type=MESH,
                )
                copy.start()
                copies.append(copy)
            for slot, peer in others:
                pltpu.make_async_remote_copy(
                    src_ref=stage.at[slot],
                    dst_ref=stage.at[slot],
                    send_sem=sends.at[0],
                    recv_sem=recvs.at[slot],
                    device_id=peer,
                    device_id_type=MESH,
                ).wait_recv()
            total = stage[0]
            for k in range(1, stage.shape[0]):
                total = total + stage[k]
            sent.extend(copies)
            return total

        others_a = [(xs[r] * nc + c, row_own[r]) for r in range(1, nx)]
        others_a += [(xs[r] * nc + 1 - c, row_partner[r]) for r in range(nx)]
        tile = exchange(stage_a, a_send, a_recv, x * nc + c, others_a, tile)
        others_b = list(zip(slots_b, peers_b))
        tile = exchange(stage_b, b_send, b_recv, q, others_b, tile)

        def column(index):
            return jnp.sum(jnp.where(tile_lane == index, tile, 0.0), axis=1, keepdims=True)

        population = column(krylov + 2)[:1]
        products = column(krylov)
        energy = column(krylov + 1)[:1]
        coefficients = products / population
        tile_row = lax.broadcasted_iota(jnp.int32, (krylov, lanes), 0)
        spread = jnp.sum(
            jnp.where(tile_lane == tile_row, coefficients, 0.0), axis=0, keepdims=True
        )
        gram = jnp.where(tile_lane < krylov, tile, 0.0)
        curvature = full_sum(gram * coefficients * spread)
        squares = energy - 2.0 * full_sum(coefficients * products) + curvature
        scale = jnp.sqrt(squares / population + epsilon)
        residue = image
        for j in range(krylov):
            residue = residue - coefficients[j : j + 1] * masked[j]
        vec_ref[...] = residue / scale
        lane_row = lax.broadcasted_iota(jnp.int32, (1, lanes), 1)
        hess_ref[...] = jnp.where(lane_row == krylov, scale, spread)

        for copy in sent:
            copy.wait_send()

    vmem = pl.BlockSpec(memory_space=pltpu.VMEM)
    smem = pl.BlockSpec(memory_space=pltpu.SMEM)
    anywhere = pl.BlockSpec(memory_space=pl.ANY)
    dma = pltpu.SemaphoreType.DMA
    slots = 3 * nx
    n_sends = 3 * nx
    return pl.pallas_call(
        kernel,
        out_shape=(
            jax.ShapeDtypeStruct((leaves, panels), f32),
            jax.ShapeDtypeStruct((1, lanes), f32),
        ),
        in_specs=[vmem, vmem, vmem, smem, smem, vmem, vmem, anywhere, anywhere, anywhere],
        out_specs=(vmem, vmem),
        scratch_shapes=[
            pltpu.VMEM((terms, leaves, panels), bf16),
            pltpu.VMEM((terms, leaves, panels), bf16),
            pltpu.VMEM((terms, offsets, terms), bf16),
            pltpu.VMEM((slots, 5, leaves, panels), f32),
            pltpu.VMEM((slots, leaves, lanes), f32),
            pltpu.VMEM((leaves, far_pad), jnp.int32),
            pltpu.VMEM((leaves, far_pad), jnp.int32),
            pltpu.VMEM((leaves, off_pad, wide), bf16),
            pltpu.VMEM((leaves * off_step, lanes), f32),
            pltpu.VMEM((leaves, panels, lanes), bf16),
            pltpu.VMEM((window, row_step, panels), f32),
            pltpu.VMEM((leaves * part_step, panels), f32),
            pltpu.VMEM((panels, lanes), f32),
            pltpu.VMEM((leaves // group, folded_rows, lanes), f32),
            pltpu.VMEM((leaves // group, folded_rows, lanes), f32),
            pltpu.VMEM((buffers, folded_rows, lanes), f32),
            pltpu.VMEM((offsets, lanes, lanes), bf16),
            pltpu.VMEM((group_a, krylov, lanes), f32),
            pltpu.VMEM((group_b, krylov, lanes), f32),
            dma((3,)),
            dma((n_sends,)),
            dma((slots,)),
            dma((n_sends,)),
            dma((slots,)),
            dma((group_a,)),
            dma((group_a,)),
            dma((group_b,)),
            dma((group_b,)),
        ],
        compiler_params=pltpu.CompilerParams(
            collective_id=0, has_side_effects=True, vmem_limit_bytes=56 * 1024 * 1024
        ),
    )


def solution(mesh):
    torus = Mesh(mesh.devices.reshape(4, 4, 2, mesh.shape["grp"]), AXES)
    every = AXES

    def on_device(basis, coords, areas, p2m, l2p, m2l, counts, near_list, far_list, far_offset):
        krylov, leaves, panels = basis.shape
        step = make_step(
            torus.devices.shape, krylov, leaves, panels, p2m.shape[1], m2l.shape[0],
            near_list.shape[1], far_list.shape[1],
        )
        vector, hessenberg = step(
            basis, coords.transpose(1, 0, 2), areas, counts, near_list, far_list, far_offset,
            p2m.transpose(1, 0, 2), l2p.transpose(2, 0, 1), m2l.transpose(1, 0, 2),
        )
        return vector, hessenberg[0, : krylov + 1]

    in_specs = (
        P(None, every, None),
        P(every, None, None),
        P(every, None),
        P(every, None, None),
        P(every, None, None),
        P(),
        P(every),
        P(every, None),
        P(every, None),
        P(every, None),
    )
    out_specs = (P(every, None), P())
    return jax.shard_map(
        on_device, mesh=torus, in_specs=in_specs, out_specs=out_specs, check_vma=False
    )
```

```python
import math

import jax
import jax.numpy as jnp
from jax import lax
from jax.experimental import pallas as pl
from jax.experimental.pallas import tpu as pltpu
from jax.sharding import Mesh
from jax.sharding import PartitionSpec as P

Y, Z, C, X = "seg_0", "seg_1", "seg_2", "grp"
AXES = (Y, Z, C, X)
MESH = pl.DeviceIdType.MESH
NT = (((1,), (1,)), ((), ()))
NN = (((1,), (0,)), ((), ()))
four_pi = 12.566370614359172
epsilon = 1e-06
f32 = jnp.float32
bf16 = jnp.bfloat16


def round_up(value, step):
    return -(-value // step) * step


def high_low(value):
    high = value.astype(bf16).astype(f32)
    return high, value - high


def two_parts(value):
    high, low = high_low(value)
    return high, low.astype(bf16).astype(f32)


def make_step(sizes, krylov, leaves, panels, terms, offsets, near, far):
    ny, nz, nc, nx = sizes
    segments = ny * nz * nc
    window = 3 * nx * leaves
    wide = round_up(window, 128)
    off_pad = round_up(offsets, 16)
    off_step = off_pad + 4
    far_pad = round_up(far, 128)
    lanes = 128
    group_a = nx * nc
    group_b = ny * nz
    rows = 16
    row_step = 24
    part_step = 40
    group = 8
    leaf_step = group + 1
    folded_rows = round_up((lanes - 1) * leaf_step + group, 8)
    buffers = 8

    def kernel(
        basis_ref, coords_ref, areas_ref, counts_ref, near_ref, far_ref, off_ref,
        p2m_hbm, l2p_hbm, m2l_hbm,
        vec_ref, hess_ref,
        p2m_v, l2p_v, m2l_v, panels_v, poles_v, far_v, off_v, count_v, sum_v, left_v,
        right_v, part_v, near_v, p2m_f, l2p_f, m2l_f, pair_v, stage_a, stage_b,
        load_sem, pole_send, pole_recv, panel_send, panel_recv, a_send, a_recv, b_send, b_recv,
    ):
        y, z, c, x = (lax.axis_index(name) for name in AXES)
        ys = [y] + [lax.rem(y + k, ny) for k in range(1, ny)]
        zs = [z] + [lax.rem(z + k, nz) for k in range(1, nz)]
        xs = [x] + [lax.rem(x + k, nx) for k in range(1, nx)]
        q = y * nz + z
        seg = q * nc + c
        q_across = lax.rem(q + group_b - 1 + 2 * c, group_b)
        y_across, z_across = q_across // nz, lax.rem(q_across, nz)

        loads = [
            pltpu.make_async_copy(src, dst, load_sem.at[k])
            for k, (src, dst) in enumerate(((p2m_hbm, p2m_v), (m2l_hbm, m2l_v), (l2p_hbm, l2p_v)))
        ]
        for load in loads:
            load.start()

        partner = (y, z, 1 - c, x)
        across = (y_across, z_across, 1 - c, x)
        row_own = [(y, z, c, other) for other in xs]
        row_partner = [(y, z, 1 - c, other) for other in xs]
        row_across = [(y_across, z_across, 1 - c, other) for other in xs]
        peers_b = [(other_y, other_z, c, x) for other_y in ys for other_z in zs][1:]
        slots_b = [other_y * nz + other_z for other_y in ys for other_z in zs][1:]

        barrier = pltpu.get_barrier_semaphore()
        everyone = row_own[1:] + row_partner + row_across + peers_b
        for peer in everyone:
            pl.semaphore_signal(barrier, inc=1, device_id=peer, device_id_type=MESH)

        slot_rows = lax.broadcasted_iota(jnp.int32, (leaves, panels), 0)
        mask = (slot_rows < counts_ref[0]).astype(f32)
        current = basis_ref[krylov - 1] * mask
        own = nx + x
        for comp in range(3):
            panels_v[own, comp] = coords_ref[comp]
        panels_v[own, 3] = areas_ref[...]
        panels_v[own, 4] = current

        pattern = (lax.broadcasted_iota(jnp.int32, (window, rows, panels), 1) == 6).astype(f32)
        right_v[:, :rows, :] = pattern
        for scratch in (l2p_f, m2l_f):
            scratch[...] = jnp.zeros(scratch.shape, f32)


        pl.semaphore_wait(barrier, len(everyone))

        def send(buffer, sends, recvs, number, source, target_slot, peer):
            copy = pltpu.make_async_remote_copy(
                src_ref=buffer.at[source],
                dst_ref=buffer.at[target_slot],
                send_sem=sends.at[number],
                recv_sem=recvs.at[target_slot],
                device_id=peer,
                device_id_type=MESH,
            )
            copy.start()
            return copy

        sent = []

        slot_partner = 2 * nx * c
        slot_across = 2 * nx * (1 - c)

        def pole_sends():
            for k in range(nx):
                buffers = (poles_v, pole_send, pole_recv)
                if k:
                    sent.append(send(*buffers, k - 1, own, own, row_own[k]))
                sent.append(send(*buffers, nx - 1 + k, own, slot_partner + x, row_partner[k]))
                sent.append(send(*buffers, 2 * nx - 1 + k, own, slot_across + x, row_across[k]))

        def panel_sends():
            buffers = (panels_v, panel_send, panel_recv)
            for k in (nx // 2, 1, nx - 1):
                sent.append(send(*buffers, k - 1, own, own, row_own[k]))
            sent.append(send(*buffers, nx - 1, own, slot_partner + x, partner))
            sent.append(send(*buffers, nx, own, slot_across + x, across))

        def received(buffer, sends, recvs, slot):
            pltpu.make_async_remote_copy(
                src_ref=buffer.at[slot],
                dst_ref=buffer.at[slot],
                send_sem=sends.at[0],
                recv_sem=recvs.at[slot],
                device_id=partner,
                device_id_type=MESH,
            ).wait_recv()

        def forward(r):
            buffers = (panels_v, panel_send, panel_recv)
            received(*buffers, nx + xs[r])
            base = nx + 1 + 2 * (r - 1)
            sent.append(send(*buffers, base + 1, nx + xs[r], slot_across + xs[r], across))
            sent.append(send(*buffers, base, nx + xs[r], slot_partner + xs[r], partner))

        pole_set = (poles_v, pole_send, pole_recv)
        panel_set = (panels_v, panel_send, panel_recv)
        panel_sends()

        padded = round_up(leaves, 16)

        def tall(value):
            extra = jnp.zeros((padded - leaves, value.shape[1]), f32)
            return jnp.concatenate([value, extra], axis=0).astype(bf16)

        rounded = tall(current)
        loads[0].wait()

        def unfold(source, scratch, part, count):
            start = part * group
            if not isinstance(part, int):
                start = pl.multiple_of(start, group)
            block = source[:, pl.ds(start, count), :].astype(f32)
            width = block.shape[2]
            for k in range(block.shape[0]):
                scratch[k * leaf_step : k * leaf_step + count, :width] = block[k]

        def unfolded(scratch, k):
            return scratch[pl.ds(k, lanes, stride=leaf_step), :].astype(bf16)

        def per_leaf(values, source, scratch, dims, running):
            for part in range(leaves // group):
                unfold(source, scratch.at[part], part, group)
            for part in range(leaves // group):
                for k in range(group):
                    product = lax.dot_general(
                        values, unfolded(scratch.at[part], k), dims, preferred_element_type=f32
                    )
                    row = lax.broadcasted_iota(jnp.int32, product.shape, 0)
                    running = jnp.where(row == part * group + k, product, running)
            return running

        blank = jnp.zeros((padded, lanes), f32)
        multipoles = per_leaf(rounded, p2m_v, p2m_f, NT, blank)
        poles_v[own] = jnp.zeros((leaves, lanes), f32)
        poles_v[own, :, :terms] = multipoles[:leaves, :terms]

        pole_sends()

        far_v[...] = jnp.full(far_v.shape, -1, jnp.int32)
        off_v[...] = jnp.full(off_v.shape, -1, jnp.int32)
        far_v[:, :far] = far_ref[...]
        off_v[:, :far] = off_ref[...]

        def to_counts(t, carry):
            off_row = jnp.broadcast_to(off_v[pl.ds(t, 1), :], (off_pad, far_pad))
            far_row = jnp.broadcast_to(far_v[pl.ds(t, 1), :], (wide, far_pad))
            off_hot = lax.broadcasted_iota(jnp.int32, (off_pad, far_pad), 0) == off_row
            far_hot = lax.broadcasted_iota(jnp.int32, (wide, far_pad), 0) == far_row
            pairs = lax.dot_general(
                jnp.where(off_hot, 1.0, 0.0).astype(bf16),
                jnp.where(far_hot, 1.0, 0.0).astype(bf16),
                NT,
                preferred_element_type=f32,
            )
            count_v[t] = pairs.astype(bf16)
            return carry

        lax.fori_loop(0, leaves, to_counts, 0, unroll=6)

        left_v[...] = jnp.zeros(left_v.shape, bf16)
        own_comps = [panels_v[own, comp] - 2.0 for comp in range(3)]
        splits = [two_parts(value) for value in own_comps]
        norm = sum((value[0] + value[1]) * (value[0] + value[1]) for value in splits)
        norm_high, norm_low = high_low(norm)
        one = jnp.ones((leaves, panels), f32)
        zero = jnp.zeros((leaves, panels), f32)
        highs = [-2.0 * value[0] for value in splits]
        lows = [-2.0 * value[1] for value in splits]
        columns = highs + [one, one, one, norm_high, zero]
        columns += highs + [zero] * 5
        columns += lows + [zero, zero, zero, norm_low, zero]
        columns += lows + [zero] * 5
        for k, column in enumerate(columns):
            part_v[pl.ds(k, leaves, stride=part_step), :] = column

        def to_left(t, carry):
            block = part_v[pl.ds(pl.multiple_of(t * part_step, 8), 2 * rows), :]
            left_v[t, :, : 2 * rows] = block.T.astype(bf16)
            return carry

        lax.fori_loop(0, leaves, to_left, 0, unroll=4)
        tile_lane = lax.broadcasted_iota(jnp.int32, (krylov, lanes), 1)
        masked = [basis_ref[j] * mask for j in range(krylov)]

        def folded(value):
            return sum(value[8 * k : 8 * k + 8] for k in range(leaves // 8))

        def full_sum(value):
            return jnp.sum(jnp.sum(value, axis=0, keepdims=True), axis=1, keepdims=True)

        def inner_products(vector):
            lines = [
                jnp.sum(folded(masked[i] * vector), axis=0, keepdims=True) for i in range(krylov)
            ]
            return jnp.sum(jnp.concatenate(lines, axis=0), axis=1, keepdims=True)

        tile = jnp.zeros((krylov, lanes), f32)
        for j in range(krylov):
            tile = jnp.where(tile_lane == j, inner_products(masked[j]), tile)
        tile = jnp.where(tile_lane == krylov + 2, full_sum(folded(mask)), tile)

        forward(1)
        valid_before = (seg > 0).astype(f32)
        valid_after = (seg < segments - 1).astype(f32)

        def to_right(slot):
            parts = [two_parts(panels_v[slot, comp] - 2.0) for comp in range(3)]
            area = panels_v[slot, 3]
            weight = area * panels_v[slot, 4] * (1.0 / four_pi)
            if slot < nx:
                weight = weight * valid_before
            if slot >= 2 * nx:
                weight = weight * valid_after
            square = sum((value[0] + value[1]) * (value[0] + value[1]) for value in parts)
            first, rest = high_low(square + area)
            second, third = high_low(rest)
            lines = [value[0] for value in parts] + [first, second, third]
            lines = list(enumerate(lines)) + [(7, weight)]
            lines += [(8 + k, value[1]) for k, value in enumerate(parts)]
            flat = right_v.reshape(window * row_step, panels)
            for k, line in lines:
                flat[pl.ds(slot * leaves * row_step + k, leaves, stride=row_step), :] = line

        loads[1].wait()

        def set_apart(part, buffer, count):
            scratch = m2l_f.at[buffer]
            unfold(m2l_v, scratch, part, count)
            for k in range(count):
                pair_v[part * group + k] = unfolded(scratch, k).T

        def set_apart_all(step, carry):
            for buffer in range(buffers):
                set_apart(buffers * step + buffer, buffer, group)
            return carry

        whole = offsets // group
        steps = whole // buffers
        lax.fori_loop(0, steps // 2, set_apart_all, 0)
        forward(nx - 1)
        forward(nx // 2)
        for slot in range(nx, 2 * nx):
            to_right(slot)
        lax.fori_loop(steps // 2, steps, set_apart_all, 0)
        for part in range(steps * buffers, whole):
            set_apart(part, part % buffers, group)
        if offsets % group:
            set_apart(whole, whole % buffers, offsets % group)

        def outside_slots(recv):
            for k in range(nx):
                recv(k)
                recv(2 * nx + k)

        for r in range(1, nx):
            received(*pole_set, nx + xs[r])
        outside_slots(lambda slot: received(*pole_set, slot))

        pole_parts = []
        for slot in range(3 * nx):
            value = poles_v[slot]
            if slot < nx:
                value = value * valid_before
            if slot >= 2 * nx:
                value = value * valid_after
            pole_parts.append(value)
        pole_parts.append(jnp.zeros((wide - window, lanes), f32))
        all_poles = jnp.concatenate(pole_parts, axis=0)
        pole_high, pole_low = high_low(all_poles)
        both_poles = jnp.concatenate([pole_high, pole_low], axis=1).astype(bf16)

        def to_sums(t, carry):
            both = jnp.dot(count_v[t], both_poles, preferred_element_type=f32)
            sum_v[pl.ds(t * off_step, off_pad), :] = both[:, :lanes] + both[:, lanes:]
            return carry

        lax.fori_loop(0, leaves, to_sums, 0, unroll=12)

        def to_local(first, count):
            lefts, rights = [], []
            for o in range(first, first + count):
                high, low = high_low(sum_v[pl.ds(o, leaves, stride=off_step), :])
                lefts.append(jnp.concatenate([high, low], axis=0).astype(bf16))
                rights.append(pair_v[o])
            return lax.dot_general(
                jnp.concatenate(lefts, axis=1),
                jnp.concatenate(rights, axis=0),
                NN,
                preferred_element_type=f32,
            )

        half = round_up(offsets // 2, 2)
        both = to_local(0, half) + to_local(half, offsets - half)
        inside = lax.broadcasted_iota(jnp.int32, (leaves, lanes), 1) < terms
        local = tall(jnp.where(inside, both[:leaves] + both[leaves:], 0.0))
        loads[2].wait()
        distant = per_leaf(local, l2p_v, l2p_f, NN, blank)[:leaves]

        outside_slots(lambda slot: received(*panel_set, slot))

        for slot in [*range(nx), *range(2 * nx, 3 * nx)]:
            to_right(slot)

        near_v[...] = jnp.zeros(near_v.shape, f32)
        pair_lane = lax.broadcasted_iota(jnp.int32, (panels, lanes), 1)

        def to_near(t, carry):
            left = left_v[t]
            running = jnp.zeros((panels, panels), f32)
            for start in range(0, near, 2):
                entries = [near_ref[t, n] for n in range(start, min(start + 2, near))]
                blocks = []
                for w in entries:
                    block = right_v[w, :rows, :].astype(bf16)
                    fill = jnp.zeros((lanes - 2 * rows, panels), bf16)
                    blocks.append(jnp.concatenate([block, block, fill], axis=0))
                right = jnp.concatenate(blocks, axis=1) if len(blocks) > 1 else blocks[0]
                square = jnp.dot(left, right, preferred_element_type=f32)
                for k, w in enumerate(entries):
                    inverse = lax.rsqrt(square[:, k * panels : (k + 1) * panels])
                    running = running + inverse * right_v[w, 7:8, :]
            total = jnp.sum(running, axis=1, keepdims=True)
            near_v[...] = jnp.where(pair_lane == t, total, near_v[...])
            return carry

        lax.fori_loop(0, leaves, to_near, 0, unroll=12)
        nearby = near_v[...].T[:leaves]

        image = (0.5 * current + nearby + distant) * mask
        tile = jnp.where(tile_lane == krylov, inner_products(image), tile)
        tile = jnp.where(tile_lane == krylov + 1, full_sum(folded(image * image)), tile)

        def exchange(stage, sends, recvs, me, others, value):
            stage[me] = value
            copies = []
            for k, (slot, peer) in enumerate(others):
                copy = pltpu.make_async_remote_copy(
                    src_ref=stage.at[me],
                    dst_ref=stage.at[me],
                    send_sem=sends.at[k],
                    recv_sem=recvs.at[me],
                    device_id=peer,
                    device_id_type=MESH,
                )
                copy.start()
                copies.append(copy)
            for slot, peer in others:
                pltpu.make_async_remote_copy(
                    src_ref=stage.at[slot],
                    dst_ref=stage.at[slot],
                    send_sem=sends.at[0],
                    recv_sem=recvs.at[slot],
                    device_id=peer,
                    device_id_type=MESH,
                ).wait_recv()
            total = stage[0]
            for k in range(1, stage.shape[0]):
                total = total + stage[k]
            sent.extend(copies)
            return total

        others_a = [(xs[r] * nc + c, row_own[r]) for r in range(1, nx)]
        others_a += [(xs[r] * nc + 1 - c, row_partner[r]) for r in range(nx)]
        tile = exchange(stage_a, a_send, a_recv, x * nc + c, others_a, tile)
        others_b = list(zip(slots_b, peers_b))
        tile = exchange(stage_b, b_send, b_recv, q, others_b, tile)

        def column(index):
            return jnp.sum(jnp.where(tile_lane == index, tile, 0.0), axis=1, keepdims=True)

        population = column(krylov + 2)[:1]
        products = column(krylov)
        energy = column(krylov + 1)[:1]
        coefficients = products / population
        tile_row = lax.broadcasted_iota(jnp.int32, (krylov, lanes), 0)
        spread = jnp.sum(
            jnp.where(tile_lane == tile_row, coefficients, 0.0), axis=0, keepdims=True
        )
        gram = jnp.where(tile_lane < krylov, tile, 0.0)
        curvature = full_sum(gram * coefficients * spread)
        squares = energy - 2.0 * full_sum(coefficients * products) + curvature
        scale = jnp.sqrt(squares / population + epsilon)
        residue = image
        for j in range(krylov):
            residue = residue - coefficients[j : j + 1] * masked[j]
        vec_ref[...] = residue / scale
        lane_row = lax.broadcasted_iota(jnp.int32, (1, lanes), 1)
        hess_ref[...] = jnp.where(lane_row == krylov, scale, spread)

        for copy in sent:
            copy.wait_send()

    vmem = pl.BlockSpec(memory_space=pltpu.VMEM)
    smem = pl.BlockSpec(memory_space=pltpu.SMEM)
    anywhere = pl.BlockSpec(memory_space=pl.ANY)
    dma = pltpu.SemaphoreType.DMA
    slots = 3 * nx
    n_sends = 3 * nx
    return pl.pallas_call(
        kernel,
        out_shape=(
            jax.ShapeDtypeStruct((leaves, panels), f32),
            jax.ShapeDtypeStruct((1, lanes), f32),
        ),
        in_specs=[vmem, vmem, vmem, smem, smem, vmem, vmem, anywhere, anywhere, anywhere],
        out_specs=(vmem, vmem),
        scratch_shapes=[
            pltpu.VMEM((terms, leaves, panels), bf16),
            pltpu.VMEM((terms, leaves, panels), bf16),
            pltpu.VMEM((terms, offsets, terms), bf16),
            pltpu.VMEM((slots, 5, leaves, panels), f32),
            pltpu.VMEM((slots, leaves, lanes), f32),
            pltpu.VMEM((leaves, far_pad), jnp.int32),
            pltpu.VMEM((leaves, far_pad), jnp.int32),
            pltpu.VMEM((leaves, off_pad, wide), bf16),
            pltpu.VMEM((leaves * off_step, lanes), f32),
            pltpu.VMEM((leaves, panels, lanes), bf16),
            pltpu.VMEM((window, row_step, panels), f32),
            pltpu.VMEM((leaves * part_step, panels), f32),
            pltpu.VMEM((panels, lanes), f32),
            pltpu.VMEM((leaves // group, folded_rows, lanes), f32),
            pltpu.VMEM((leaves // group, folded_rows, lanes), f32),
            pltpu.VMEM((buffers, folded_rows, lanes), f32),
            pltpu.VMEM((offsets, lanes, lanes), bf16),
            pltpu.VMEM((group_a, krylov, lanes), f32),
            pltpu.VMEM((group_b, krylov, lanes), f32),
            dma((3,)),
            dma((n_sends,)),
            dma((slots,)),
            dma((n_sends,)),
            dma((slots,)),
            dma((group_a,)),
            dma((group_a,)),
            dma((group_b,)),
            dma((group_b,)),
        ],
        compiler_params=pltpu.CompilerParams(
            collective_id=0, has_side_effects=True, vmem_limit_bytes=56 * 1024 * 1024
        ),
    )


def solution(mesh):
    torus = Mesh(mesh.devices.reshape(4, 4, 2, mesh.shape["grp"]), AXES)
    every = AXES

    def on_device(basis, coords, areas, p2m, l2p, m2l, counts, near_list, far_list, far_offset):
        krylov, leaves, panels = basis.shape
        step = make_step(
            torus.devices.shape, krylov, leaves, panels, p2m.shape[1], m2l.shape[0],
            near_list.shape[1], far_list.shape[1],
        )
        vector, hessenberg = step(
            basis, coords.transpose(1, 0, 2), areas, counts, near_list, far_list, far_offset,
            p2m.transpose(1, 0, 2), l2p.transpose(2, 0, 1), m2l.transpose(1, 0, 2),
        )
        return vector, hessenberg[0, : krylov + 1]

    in_specs = (
        P(None, every, None),
        P(every, None, None),
        P(every, None),
        P(every, None, None),
        P(every, None, None),
        P(),
        P(every),
        P(every, None),
        P(every, None),
        P(every, None),
    )
    out_specs = (P(every, None), P())
    return jax.shard_map(
        on_device, mesh=torus, in_specs=in_specs, out_specs=out_specs, check_vma=False
    )
```
